32 devices in a mesh: gx: 8 (over z, core), gy: 4 (over y, x).
Axes of the slice: x: 2, y: 2, z: 4, core: 2. Of those that a mesh axis runs over, the one named last changes fastest.
Arguments:
- potential: float32 [32, 64, 256], P('gx', 'gy'), may hold values from -0.2 to 1.2
- recovery: float32 [32, 64, 256], P('gx', 'gy'), may hold values from 0 to 1.5
- fiber_angles: float32 [2, 32, 64, 256], P(None, 'gx', 'gy'), may hold values from -3.140625 to 3.140625
- deform: float32 [9, 8192], P(None, ('gx', 'gy')), may hold values from -0.15 to 1.25, as said below
- elem_slot: int32 [8, 16, 64], P('gx', 'gy'), may hold values from 0 to 8191, as said below
Outputs:
- potential_next: float32 [32, 64, 256], P('gx', 'gy')
- recovery_next: float32 [32, 64, 256], P('gx', 'gy')
The draws below stay inside these ranges and needn't reach their ends.
Inputs may be any that keep to these rules, and one draw needn't show every extreme that they name: `elem_slot`: entries are distinct. Slot s lies on device s / 256 (rounded down) of gx+gy. The elements of one device's block along gx and gy lie in the slots of the devices with the same index along gx, exactly 64 of them in each. `deform`: components 0, 4 and 8 (the diagonal of F) lie in 0.8 to 1.25, the other six in -0.15 to 0.15.
All inputs are finite; a program needn't handle non-finite values.
Results may differ from the reference program's by a relative error of at most 0.0003.
Values sent between devices are 32-bit elements; how exact they have to be, the bound alone decides.
No kernel may reach another device: no remote copies, remote signals or barrier semaphores. Data moves between devices by JAX's collectives and lax.ppermute only.
A program may use at most 64 MiB of HBM per device.

```python
import math
import jax
import jax.numpy as jnp
from jax import lax

RATIO = 4
KX = 1
KY = 4
NCZ = 64
NZ = 256
NX = 32
NY = 64
CB = 256
SHARE = 64
NE = 8192
N_GX = 8
N_GY = 4
DEVICES = 32


def draw_deform(key, part):
    diag_key = jax.random.fold_in(key, 21)
    off_key = jax.random.fold_in(key, 22)
    diagonal = jnp.exp(jax.random.uniform(diag_key, (3, NE), jnp.float32, math.log(0.8), math.log(1.25)))
    offside = jnp.clip(0.06 * jax.random.normal(off_key, (6, NE), jnp.float32), -0.15, 0.15)
    diagonal = jnp.clip(diagonal, 0.8, 1.25)
    rows = [diagonal[0], offside[0], offside[1], offside[2], diagonal[1], offside[3], offside[4], offside[5], diagonal[2]]
    return jnp.stack(rows).astype(jnp.float32)


def draw_elem_slot(key, part):
    block_keys = jax.random.split(jax.random.fold_in(key, 31), DEVICES)
    holder_keys = jax.random.split(jax.random.fold_in(key, 32), DEVICES)
    ranks = jax.vmap(lambda one_key: jax.random.permutation(one_key, CB))(block_keys).astype(jnp.int32)
    holding = jax.vmap(lambda one_key: jax.random.permutation(one_key, CB))(holder_keys).astype(jnp.int32)
    device_index = jnp.arange(DEVICES, dtype=jnp.int32)
    row_start = device_index // N_GY * N_GY
    column = device_index % N_GY
    holder = row_start[:, None] + ranks // SHARE
    position = column[:, None] * SHARE + ranks % SHARE
    local_slot = holding[holder, position]
    slots = holder * CB + local_slot
    grid = slots.reshape(N_GX, N_GY, KX, KY, NCZ).transpose(0, 2, 1, 3, 4).reshape(N_GX * KX, N_GY * KY, NCZ)
    return grid.astype(jnp.int32)


def block_scale(key, dims, shards, smallest, largest):
    def one(dim, parts):
        draws = jax.random.uniform(jax.random.fold_in(jax.random.fold_in(key, 6), dim), (parts,), jnp.float32, smallest / len(shards), largest / len(shards))
        return jnp.repeat(jnp.exp(draws), dims[dim] // parts).reshape((-1,) + (1,) * (len(dims) - dim - 1))

    level = one(*shards[0])
    for cut in shards[1:]:
        level = level * one(*cut)
    return level


def setup_inputs(seed: int = 0) -> dict:
    seeds = jax.random.split(jax.random.key(seed), 6)
    potential = jnp.clip(-0.2 + 1.4000001 * jax.random.uniform(seeds[0], (NX, NY, NZ), jnp.float32) ** block_scale(seeds[0], (NX, NY, NZ), ((0, 8), (1, 4)), -0.2, 0.2), -0.2, 1.2)
    recovery = jnp.clip(1.5 * jax.random.uniform(seeds[1], (NX, NY, NZ), jnp.float32) ** block_scale(seeds[1], (NX, NY, NZ), ((0, 8), (1, 4)), -0.2, 0.2), 0.0, 1.5)
    fiber_angles = jnp.clip(jax.random.uniform(seeds[2], (2, NX, NY, NZ), jnp.float32, -3.140625, 3.140625), -3.140625, 3.140625)
    deform = draw_deform(jax.random.fold_in(seeds[5], 71), 0)
    elem_slot = draw_elem_slot(jax.random.fold_in(seeds[5], 71), 0)
    return dict(potential=potential, recovery=recovery, fiber_angles=fiber_angles, deform=deform, elem_slot=elem_slot)


sigma_fiber = 1.0
sigma_cross = 0.3
time_step = 0.1
excite_gain = 8.0
excite_level = 0.15
stretch_gain = 10.0
stretch_reversal = 0.6
recover_rate = 0.5

def refine(padded, dim):
    inner_size = padded.shape[dim] - 2
    lower = lax.slice_in_dim(padded, 0, inner_size, axis=dim)
    middle = lax.slice_in_dim(padded, 1, inner_size + 1, axis=dim)
    upper = lax.slice_in_dim(padded, 2, inner_size + 2, axis=dim)
    pieces = []
    for position in range(RATIO):
        offset = (position + 0.5) / RATIO - 0.5
        weight = abs(offset)
        neighbor = lower if offset < 0 else upper
        pieces.append((1.0 - weight) * middle + weight * neighbor)
    stacked = jnp.stack(pieces, axis=dim + 1)
    new_shape = list(padded.shape)
    new_shape[dim] = inner_size * RATIO
    return stacked.reshape(new_shape)

def directions(angles):
    azimuth = angles[0]
    elevation = angles[1]
    return jnp.stack([jnp.cos(azimuth) * jnp.cos(elevation), jnp.sin(azimuth) * jnp.cos(elevation), jnp.sin(elevation)])

def tensors(field, fiber):
    entries = [field[number] for number in range(9)]

    def element(row_index, col_index):
        return entries[3 * (row_index % 3) + col_index % 3]
    cofactor = [[element(row_index + 1, col_index + 1) * element(row_index + 2, col_index + 2) - element(row_index + 1, col_index + 2) * element(row_index + 2, col_index + 1) for col_index in range(3)] for row_index in range(3)]
    determinant = element(0, 0) * cofactor[0][0] + element(0, 1) * cofactor[0][1] + element(0, 2) * cofactor[0][2]
    inverse = [[cofactor[col_index][row_index] / determinant for col_index in range(3)] for row_index in range(3)]
    stretched = [element(row_index, 0) * fiber[0] + element(row_index, 1) * fiber[1] + element(row_index, 2) * fiber[2] for row_index in range(3)]
    stretch = jnp.sqrt(stretched[0] * stretched[0] + stretched[1] * stretched[1] + stretched[2] * stretched[2])
    pulled = [inverse[row_index][0] * fiber[0] + inverse[row_index][1] * fiber[1] + inverse[row_index][2] * fiber[2] for row_index in range(3)]
    conduct = []
    for first_index, second_index in ((0, 0), (1, 1), (2, 2), (0, 1), (0, 2), (1, 2)):
        metric = inverse[first_index][0] * inverse[second_index][0] + inverse[first_index][1] * inverse[second_index][1] + inverse[first_index][2] * inverse[second_index][2]
        conduct.append(sigma_cross * metric + (sigma_fiber - sigma_cross) * pulled[first_index] * pulled[second_index])
    return (jnp.stack(conduct), stretch)

def close_faces(flux, dim, at_first, at_last):
    extent = flux.shape[dim]
    face_index = lax.broadcasted_iota(jnp.int32, flux.shape, dim)
    closed = (face_index == 0) & at_first | (face_index == extent - 1) & at_last
    return jnp.where(closed, jnp.zeros_like(flux), flux)

def divergence(potential_pad, tensor_pad, first_x, last_x, first_y, last_y):
    grad_x = (potential_pad[2:, :, :] - potential_pad[:-2, :, :]) * 0.5
    grad_y = (potential_pad[:, 2:, :] - potential_pad[:, :-2, :]) * 0.5
    grad_z = (potential_pad[:, :, 2:] - potential_pad[:, :, :-2]) * 0.5

    def face_mean(component, dim):
        inner = tensor_pad[component]
        if dim == 0:
            inner = inner[:, 1:-1, 1:-1]
        elif dim == 1:
            inner = inner[1:-1, :, 1:-1]
        else:
            inner = inner[1:-1, 1:-1, :]
        extent = inner.shape[dim]
        return (lax.slice_in_dim(inner, 1, extent, axis=dim) + lax.slice_in_dim(inner, 0, extent - 1, axis=dim)) * 0.5
    step_x = potential_pad[1:, 1:-1, 1:-1] - potential_pad[:-1, 1:-1, 1:-1]
    mean_y = (grad_y[1:, :, 1:-1] + grad_y[:-1, :, 1:-1]) * 0.5
    mean_z = (grad_z[1:, 1:-1, :] + grad_z[:-1, 1:-1, :]) * 0.5
    flux_x = face_mean(0, 0) * step_x + face_mean(3, 0) * mean_y + face_mean(4, 0) * mean_z
    flux_x = close_faces(flux_x, 0, first_x, last_x)
    step_y = potential_pad[1:-1, 1:, 1:-1] - potential_pad[1:-1, :-1, 1:-1]
    mean_x = (grad_x[:, 1:, 1:-1] + grad_x[:, :-1, 1:-1]) * 0.5
    mean_z = (grad_z[1:-1, 1:, :] + grad_z[1:-1, :-1, :]) * 0.5
    flux_y = face_mean(3, 1) * mean_x + face_mean(1, 1) * step_y + face_mean(5, 1) * mean_z
    flux_y = close_faces(flux_y, 1, first_y, last_y)
    step_z = potential_pad[1:-1, 1:-1, 1:] - potential_pad[1:-1, 1:-1, :-1]
    mean_x = (grad_x[:, 1:-1, 1:] + grad_x[:, 1:-1, :-1]) * 0.5
    mean_y = (grad_y[1:-1, :, 1:] + grad_y[1:-1, :, :-1]) * 0.5
    flux_z = face_mean(4, 2) * mean_x + face_mean(5, 2) * mean_y + face_mean(2, 2) * step_z
    flux_z = close_faces(flux_z, 2, True, True)
    return flux_x[1:] - flux_x[:-1] + (flux_y[:, 1:] - flux_y[:, :-1]) + (flux_z[:, :, 1:] - flux_z[:, :, :-1])

def update(voltage, recovery, divergent, stretch):
    current = excite_gain * voltage * (voltage - excite_level) * (voltage - 1.0) + voltage * recovery
    current = current + stretch_gain * jnp.maximum(stretch - 1.0, 0.0) * (voltage - stretch_reversal)
    voltage_next = voltage + time_step * (divergent - current)
    recovery_next = recovery + time_step * recover_rate * (-recovery - excite_gain * voltage * (voltage - excite_level - 1.0))
    return (voltage_next, recovery_next)

def reference(potential, recovery, fiber_angles, deform, elem_slot):
    coarse = deform[:, elem_slot]
    coarse = jnp.pad(coarse, ((0, 0), (1, 1), (1, 1), (1, 1)), mode='edge')
    along_x = refine(coarse, 1)
    along_x = jnp.pad(along_x, ((0, 0), (1, 1), (0, 0), (0, 0)), mode='edge')
    angles_pad = jnp.pad(fiber_angles, ((0, 0), (1, 1), (0, 0), (0, 0)), mode='edge')
    potential_all = jnp.pad(potential, 1, mode='edge')
    width = NX // N_GX

    def slab(index):
        start = (index * width).astype(jnp.int32)
        segment = lax.dynamic_slice_in_dim(along_x, start, width + 2, axis=1)
        fine_field = refine(refine(segment, 2), 3)
        angles = lax.dynamic_slice_in_dim(angles_pad, start, width + 2, axis=1)
        conduct, stretch = tensors(fine_field, directions(angles))
        tensor_pad = jnp.pad(conduct, ((0, 0), (0, 0), (1, 1), (1, 1)), mode='edge')
        potential_pad = lax.dynamic_slice_in_dim(potential_all, start, width + 2, axis=0)
        divergent = divergence(potential_pad, tensor_pad, index == 0, index == N_GX - 1, True, True)
        voltage = lax.dynamic_slice_in_dim(potential, start, width, axis=0)
        resting = lax.dynamic_slice_in_dim(recovery, start, width, axis=0)
        return update(voltage, resting, divergent, stretch[1:-1])
    voltage_next, recovery_next = lax.map(slab, jnp.arange(N_GX, dtype=jnp.int32))
    return (voltage_next.reshape(NX, NY, NZ), recovery_next.reshape(NX, NY, NZ))
```

```python
import functools

import jax
import jax.numpy as jnp
import numpy as np
from jax import lax
from jax.experimental import pallas as pl
from jax.experimental.pallas import tpu as pltpu
from jax.sharding import PartitionSpec as P

RATIO = 4

sigma_fiber = 1.0
sigma_cross = 0.3
time_step = 0.1
excite_gain = 8.0
excite_level = 0.15
stretch_gain = 10.0
stretch_reversal = 0.6
recover_rate = 0.5


def round_up(value, multiple):
    return -(-value // multiple) * multiple


def interpolation(count):
    weights = np.zeros((RATIO * count + 2, count + 2))
    for cell in range(-1, RATIO * count + 1):
        element, position = cell // RATIO, cell % RATIO
        offset = (position + 0.5) / RATIO - 0.5
        weights[cell + 1, element + 1] += 1.0 - abs(offset)
        weights[cell + 1, element + 1 + (1 if offset > 0 else -1)] += abs(offset)
    return weights


def fit_series():
    nodes = np.cos((np.arange(64) + 0.5) * np.pi / 64)
    square = (nodes + 1.0) * 0.5 * np.pi**2
    root = np.sqrt(square)
    series = []
    for values in (np.sin(root) / root, np.cos(root)):
        fitted = np.polynomial.chebyshev.Chebyshev.fit(square, values, 8, domain=[0.0, np.pi**2])
        series.append(fitted.convert(kind=np.polynomial.Polynomial).coef)
    return series


SINE, COSINE = fit_series()


def horner(series, square):
    total = jnp.full_like(square, float(series[-1]))
    for coefficient in series[-2::-1]:
        total = total * square + float(coefficient)
    return total


def sine_cosine(angle):
    square = angle * angle
    return (angle * horner(SINE, square), horner(COSINE, square))


def parts_of(values, count):
    pieces = []
    for _ in range(count):
        piece = values.astype(jnp.bfloat16)
        pieces.append(piece)
        values = values - piece.astype(jnp.float32)
    return pieces


def dot(left, right):
    return jnp.dot(left, right, preferred_element_type=jnp.float32)


def fill_gradients(out_ref, start, deform_ref, slot_ref, row, rows):
    components, held = deform_ref.shape
    columns, depth = slot_ref.shape[1:]
    out_ref[start : start + rows, :] = jnp.zeros((rows, out_ref.shape[1]), jnp.float32)
    out_ref[start : start + components, 0:held] = deform_ref[...]
    out_ref[start + components : start + components + columns, 0:depth] = slot_ref[row].astype(
        jnp.float32
    )


def pack_x(potential_ref, angle_ref, deform_ref, slot_ref, down_ref, up_ref):
    cells_x, cells_y = potential_ref.shape[:2]
    for out_ref, cell, element in (
        (down_ref, 0, 0),
        (up_ref, cells_x - 1, slot_ref.shape[0] - 1),
    ):
        out_ref[0:cells_y] = potential_ref[cell]
        out_ref[cells_y : 2 * cells_y] = angle_ref[0, cell]
        out_ref[2 * cells_y : 3 * cells_y] = angle_ref[1, cell]
        fill_gradients(
            out_ref, 3 * cells_y, deform_ref, slot_ref, element, out_ref.shape[0] - 3 * cells_y
        )


def pack_y(
    potential_ref, angle_ref, deform_ref, slot_ref, down_ref, up_ref, low_ref, high_ref, out_ref
):
    cells_x, cells_y, depth = potential_ref.shape
    rows = low_ref.shape[0] - 3 * cells_y
    elements = slot_ref.shape[0]
    at_first = lax.axis_index("gx") == 0
    at_last = lax.axis_index("gx") == lax.axis_size("gx") - 1

    def low(start, stop):
        return jnp.where(at_first, down_ref[start:stop], low_ref[start:stop])

    def high(start, stop):
        return jnp.where(at_last, up_ref[start:stop], high_ref[start:stop])

    out_ref[0:rows] = low(3 * cells_y, 3 * cells_y + rows)
    for element in range(elements):
        fill_gradients(out_ref, (element + 1) * rows, deform_ref, slot_ref, element, rows)
    out_ref[(elements + 1) * rows : (elements + 2) * rows] = high(
        3 * cells_y, 3 * cells_y + rows
    )
    base = (elements + 2) * rows
    side_rows = (out_ref.shape[0] - base) // 2
    first_rows = round_up(cells_x + 2, 8)
    out_ref[base:, :] = jnp.zeros((2 * side_rows, depth), jnp.float32)
    for side, cell in ((0, 0), (1, cells_y - 1)):
        start = base + side * side_rows
        out_ref[start : start + 1] = low(cell, cell + 1)
        for x in range(cells_x):
            out_ref[start + 1 + x : start + 2 + x] = potential_ref[x, cell : cell + 1, :]
        out_ref[start + 1 + cells_x : start + 2 + cells_x] = high(cell, cell + 1)
        for kind in range(2):
            for x in range(cells_x):
                line = start + first_rows + kind * cells_x + x
                out_ref[line : line + 1] = angle_ref[kind, x, cell : cell + 1, :]


def tensors(entries, azimuth, elevation):
    sin_u, cos_u = sine_cosine(azimuth)
    sin_e, cos_e = sine_cosine(elevation)
    fiber = [cos_u * cos_e, sin_u * cos_e, sin_e]

    def element(row_index, col_index):
        return entries[3 * (row_index % 3) + col_index % 3]

    cofactor = [
        [
            element(row + 1, col + 1) * element(row + 2, col + 2)
            - element(row + 1, col + 2) * element(row + 2, col + 1)
            for col in range(3)
        ]
        for row in range(3)
    ]
    determinant = (
        element(0, 0) * cofactor[0][0]
        + element(0, 1) * cofactor[0][1]
        + element(0, 2) * cofactor[0][2]
    )
    scale = 1.0 / determinant
    adjugate = [[cofactor[col][row] for col in range(3)] for row in range(3)]
    pulled = [
        adjugate[row][0] * fiber[0] + adjugate[row][1] * fiber[1] + adjugate[row][2] * fiber[2]
        for row in range(3)
    ]
    cross = (scale * scale) * sigma_cross
    along = (scale * scale) * (sigma_fiber - sigma_cross)
    conduct = []
    for first, second in ((0, 0), (1, 1), (2, 2), (0, 1), (0, 2), (1, 2)):
        metric = (
            adjugate[first][0] * adjugate[second][0]
            + adjugate[first][1] * adjugate[second][1]
            + adjugate[first][2] * adjugate[second][2]
        )
        conduct.append(cross * metric + along * (pulled[first] * pulled[second]))
    return conduct, fiber


def stretch_of(entries, fiber):
    total = None
    for row in range(3):
        value = (
            entries[3 * row] * fiber[0]
            + entries[3 * row + 1] * fiber[1]
            + entries[3 * row + 2] * fiber[2]
        )
        total = value * value if total is None else total + value * value
    return jnp.sqrt(total)


def step(
    potential_ref,
    recovery_ref,
    angle_ref,
    down_ref,
    up_ref,
    low_ref,
    high_ref,
    row_ref,
    deep_ref,
    wide_ref,
    potential_out,
    recovery_out,
    coarse_ref,
    fine_ref,
    conduct_ref,
    stretch_ref,
    *,
    columns,
    coarse_depth,
    held,
    components,
):
    cells_x, cells_y, depth = potential_ref.shape
    devices = row_ref.shape[0]
    rows = low_ref.shape[0] - 3 * cells_y
    elements = cells_x // RATIO
    gx = lax.axis_index("gx")
    gy = lax.axis_index("gy")
    at_first_x = gx == 0
    at_last_x = gx == lax.axis_size("gx") - 1
    at_first_y = gy == 0
    at_last_y = gy == lax.axis_size("gy") - 1
    left = jnp.where(at_first_y, gy, gy - 1)
    right = jnp.where(at_last_y, gy, gy + 1)

    lanes = 2 * coarse_depth
    lane = lax.broadcasted_iota(jnp.int32, (1, lanes), 1)
    slot_lines = []
    for r in range(elements + 2):
        base = r * rows + components
        own = row_ref[gy, base : base + columns, 0:lanes]
        before = jnp.where(
            at_first_y, own[0:1], row_ref[left, base + columns - 1 : base + columns, 0:lanes]
        )
        after = jnp.where(
            at_last_y, own[columns - 1 : columns], row_ref[right, base : base + 1, 0:lanes]
        )
        line = [before] + [own[c : c + 1] for c in range(columns)] + [after]
        slot_lines.append(line)
    count = columns + 2
    gathered = [[None] * (count // 2) for _ in range(elements + 2)]
    for r in range(elements + 2):
        table = row_ref[:, r * rows : (r + 1) * rows, 0:held].reshape(devices * rows, held)
        table_parts = parts_of(table, 3)
        for pair in range(count // 2):
            slots = jnp.where(
                lane < coarse_depth,
                slot_lines[r][2 * pair],
                pltpu.roll(slot_lines[r][2 * pair + 1], coarse_depth, 1),
            ).astype(jnp.int32)
            place = slots % held
            holder = (slots // held) % devices
            match = lax.broadcasted_iota(jnp.int32, (held, lanes), 0) == place
            chosen = jnp.where(match, 1.0, 0.0).astype(jnp.bfloat16)
            values = dot(table_parts[0], chosen)
            for part in table_parts[1:]:
                values = values + dot(part, chosen)
            picked = values[0:rows]
            for device in range(1, devices):
                picked = jnp.where(
                    holder == device, values[device * rows : (device + 1) * rows], picked
                )
            gathered[r][pair] = picked

    tall = (elements + 2) * rows
    for pair in range(count // 2):
        stacked = jnp.concatenate([gathered[r][pair] for r in range(elements + 2)], axis=0)
        values = None
        for part in parts_of(stacked, 3):
            term = dot(part, deep_ref[...])
            values = term if values is None else values + term
        coarse_ref[2 * pair * tall : (2 * pair + 1) * tall] = values[:, 0:depth]
        coarse_ref[(2 * pair + 1) * tall : (2 * pair + 2) * tall] = values[:, depth : 2 * depth]
    coarse_parts = parts_of(coarse_ref[...], 2)
    fine_ref[...] = dot(wide_ref[...], coarse_parts[0]) + dot(wide_ref[...], coarse_parts[1])

    total_rows = fine_ref.shape[0] // components
    inner_rows = cells_x * cells_y
    base_y = (elements + 2) * rows
    side_rows = (row_ref.shape[1] - base_y) // 2
    first_rows = round_up(cells_x + 2, 8)
    left_start = pl.multiple_of(jnp.where(at_first_y, base_y, base_y + side_rows), 8)
    right_start = pl.multiple_of(jnp.where(at_last_y, base_y + side_rows, base_y), 8)
    chunk = 8
    for start in range(0, total_rows, chunk):
        entries = [
            fine_ref[k * total_rows + start : k * total_rows + start + chunk]
            for k in range(components)
        ]
        if start < inner_rows:
            x, y = start // cells_y, start % cells_y
            azimuth = angle_ref[0, x, y : y + chunk]
            elevation = angle_ref[1, x, y : y + chunk]
        elif start < inner_rows + 2 * cells_y:
            is_low = start < inner_rows + cells_y
            y = (start - inner_rows) % cells_y
            kinds = []
            for kind in range(2):
                line = (1 + kind) * cells_y + y
                own_ref, got_ref = (down_ref, low_ref) if is_low else (up_ref, high_ref)
                kinds.append(
                    jnp.where(
                        at_first_x if is_low else at_last_x,
                        own_ref[line : line + chunk],
                        got_ref[line : line + chunk],
                    )
                )
            azimuth, elevation = kinds
        else:
            left_angles = row_ref[left, pl.ds(left_start + first_rows, 2 * cells_x), :]
            right_angles = row_ref[right, pl.ds(right_start + first_rows, 2 * cells_x), :]
            azimuth = jnp.concatenate([left_angles[0:cells_x], right_angles[0:cells_x]], axis=0)
            elevation = jnp.concatenate([left_angles[cells_x:], right_angles[cells_x:]], axis=0)
        conduct, fiber = tensors(entries, azimuth, elevation)
        for number in range(6):
            conduct_ref[number, start : start + chunk] = conduct[number]
        if start < inner_rows:
            stretch_ref[start : start + chunk] = stretch_of(entries, fiber)

    row_index = lax.broadcasted_iota(jnp.int32, (cells_y, depth), 0)
    lane_index = lax.broadcasted_iota(jnp.int32, (cells_y, depth), 1)
    rim_low = row_ref[left, pl.ds(left_start, first_rows), :]
    rim_high = row_ref[right, pl.ds(right_start, first_rows), :]

    def deeper(values, first):
        return jnp.where(first, values, pltpu.roll(values, 1, 1))

    def grad_z(values):
        index = lax.broadcasted_iota(jnp.int32, values.shape, 1)
        after = jnp.where(index == depth - 1, values, pltpu.roll(values, depth - 1, 1))
        before = jnp.where(index == 0, values, pltpu.roll(values, 1, 1))
        return (after - before) * 0.5

    def lower_y(values, rim):
        return jnp.where(row_index == 0, rim, pltpu.roll(values, 1, 0))

    def upper_y(values, rim):
        return jnp.where(row_index == cells_y - 1, rim, pltpu.roll(values, cells_y - 1, 0))

    def voltage_at(x):
        if x < 0:
            return jnp.where(at_first_x, down_ref[0:cells_y], low_ref[0:cells_y])
        if x >= cells_x:
            return jnp.where(at_last_x, up_ref[0:cells_y], high_ref[0:cells_y])
        return potential_ref[x]

    def conduct_at(number, x):
        if x < 0:
            return conduct_ref[number, inner_rows : inner_rows + cells_y]
        if x >= cells_x:
            return conduct_ref[number, inner_rows + cells_y : inner_rows + 2 * cells_y]
        return conduct_ref[number, x * cells_y : (x + 1) * cells_y]

    voltages = [voltage_at(x) for x in range(-1, cells_x + 1)]
    grads_y = [
        (
            upper_y(voltages[x], rim_high[x : x + 1])
            - lower_y(voltages[x], rim_low[x : x + 1])
        )
        * 0.5
        for x in range(cells_x + 2)
    ]
    grads_z = [grad_z(values) for values in voltages]
    rim_z = [grad_z(rim_low), grad_z(rim_high)]

    def flux(tensor_a, tensor_b, grads_a, grads_b, straight, voltage_a, voltage_b):
        total = None
        for place in range(3):
            mean = (tensor_a[place] + tensor_b[place]) * 0.5
            if place == straight:
                term = mean * (voltage_b - voltage_a)
            else:
                term = mean * ((grads_a[place] + grads_b[place]) * 0.5)
            total = term if total is None else total + term
        return total

    flux_x = []
    for face in range(cells_x + 1):
        value = flux(
            [conduct_at(n, face - 1) for n in (0, 3, 4)],
            [conduct_at(n, face) for n in (0, 3, 4)],
            [None, grads_y[face], grads_z[face]],
            [None, grads_y[face + 1], grads_z[face + 1]],
            0,
            voltages[face],
            voltages[face + 1],
        )
        if face == 0:
            value = jnp.where(at_first_x, 0.0, value)
        if face == cells_x:
            value = jnp.where(at_last_x, 0.0, value)
        flux_x.append(value)

    rim_start = inner_rows + 2 * cells_y
    for x in range(cells_x):
        voltage = voltages[x + 1]
        grad_x = (voltages[x + 2] - voltages[x]) * 0.5
        grad_y = grads_y[x + 1]
        grad_zz = grads_z[x + 1]
        tensor = [conduct_at(n, x) for n in (3, 1, 5)]
        low_tensor = [conduct_ref[n, rim_start + x : rim_start + x + 1] for n in (3, 1, 5)]
        high_tensor = [
            conduct_ref[n, rim_start + cells_x + x : rim_start + cells_x + x + 1]
            for n in (3, 1, 5)
        ]
        low_grads = [
            (rim_low[x + 2 : x + 3] - rim_low[x : x + 1]) * 0.5,
            None,
            rim_z[0][x + 1 : x + 2],
        ]
        high_grads = [
            (rim_high[x + 2 : x + 3] - rim_high[x : x + 1]) * 0.5,
            None,
            rim_z[1][x + 1 : x + 2],
        ]
        lower = flux(
            [lower_y(tensor[n], low_tensor[n]) for n in range(3)],
            tensor,
            [lower_y(grad_x, low_grads[0]), None, lower_y(grad_zz, low_grads[2])],
            [grad_x, None, grad_zz],
            1,
            lower_y(voltage, rim_low[x + 1 : x + 2]),
            voltage,
        )
        lower = jnp.where((row_index == 0) & at_first_y, 0.0, lower)
        top = flux(
            [value[cells_y - 1 : cells_y] for value in tensor],
            high_tensor,
            [grad_x[cells_y - 1 : cells_y], None, grad_zz[cells_y - 1 : cells_y]],
            high_grads,
            1,
            voltage[cells_y - 1 : cells_y],
            rim_high[x + 1 : x + 2],
        )
        top = jnp.where(at_last_y, 0.0, top)
        divergent = flux_x[x + 1] - flux_x[x] + (upper_y(lower, top) - lower)
        first = lane_index == 0
        tensor = [conduct_at(n, x) for n in (4, 5, 2)]
        before = flux(
            [deeper(value, first) for value in tensor],
            tensor,
            [deeper(grad_x, first), deeper(grad_y, first), None],
            [grad_x, grad_y, None],
            2,
            deeper(voltage, first),
            voltage,
        )
        before = jnp.where(first, 0.0, before)
        divergent = divergent + (pltpu.roll(before, depth - 1, 1) - before)
        recovery = recovery_ref[x]
        stretch = stretch_ref[x * cells_y : (x + 1) * cells_y]
        current = (
            excite_gain * voltage * (voltage - excite_level) * (voltage - 1.0)
            + voltage * recovery
        )
        current = current + stretch_gain * jnp.maximum(stretch - 1.0, 0.0) * (
            voltage - stretch_reversal
        )
        potential_out[x] = voltage + time_step * (divergent - current)
        recovery_out[x] = recovery + time_step * recover_rate * (
            -recovery - excite_gain * voltage * (voltage - excite_level - 1.0)
        )


def weights_of(cells_x, cells_y, columns, coarse_depth, depth, rows, components):
    elements = cells_x // RATIO
    deep = np.zeros((coarse_depth, depth))
    along_z = interpolation(coarse_depth)[1:-1]
    deep += along_z[:, 1:-1].T
    deep[0] += along_z[:, 0]
    deep[-1] += along_z[:, -1]
    pair = np.zeros((2 * coarse_depth, 2 * depth))
    pair[:coarse_depth, :depth] = deep
    pair[coarse_depth:, depth:] = deep
    along_x = interpolation(elements)
    along_y = interpolation(columns)
    places = [(x + 1, y + 1) for x in range(cells_x) for y in range(cells_y)]
    places += [(x, y + 1) for x in (0, cells_x + 1) for y in range(cells_y)]
    places += [(x + 1, y) for y in (0, cells_y + 1) for x in range(cells_x)]
    wide = np.zeros((components, len(places), columns + 2, elements + 2, rows))
    for line, (x, y) in enumerate(places):
        block = along_y[y][:, None] * along_x[x][None, :]
        for k in range(components):
            wide[k, line, :, :, k] = block
    wide = wide.reshape(components * len(places), -1)
    return jnp.asarray(pair, jnp.bfloat16), jnp.asarray(wide, jnp.bfloat16), len(places)


def local(potential, recovery, fiber_angles, deform, elem_slot):
    cells_x, cells_y, depth = potential.shape
    elements, columns, coarse_depth = elem_slot.shape
    components, held = deform.shape
    rows = round_up(components + columns, 8)
    deep, wide, line_count = weights_of(
        cells_x, cells_y, columns, coarse_depth, depth, rows, components
    )
    packet = jax.ShapeDtypeStruct((3 * cells_y + rows, depth), jnp.float32)
    down, up = pl.pallas_call(pack_x, out_shape=(packet, packet), name="pack_x")(
        potential, fiber_angles, deform, elem_slot
    )
    forward = [(i, i + 1) for i in range(lax.axis_size("gx") - 1)]
    backward = [(target, source) for source, target in forward]
    low = lax.ppermute(up, "gx", forward)
    high = lax.ppermute(down, "gx", backward)
    sides = 2 * (round_up(cells_x + 2, 8) + 2 * cells_x)
    payload = pl.pallas_call(
        pack_y,
        out_shape=jax.ShapeDtypeStruct(((elements + 2) * rows + sides, depth), jnp.float32),
        name="pack_y",
    )(potential, fiber_angles, deform, elem_slot, down, up, low, high)
    row = lax.all_gather(payload, "gy", axis=0, tiled=False)
    block = jax.ShapeDtypeStruct((cells_x, cells_y, depth), jnp.float32)
    return pl.pallas_call(
        functools.partial(
            step, columns=columns, coarse_depth=coarse_depth, held=held, components=components
        ),
        out_shape=(block, block),
        scratch_shapes=[
            pltpu.VMEM(((columns + 2) * (elements + 2) * rows, depth), jnp.float32),
            pltpu.VMEM((components * line_count, depth), jnp.float32),
            pltpu.VMEM((6, line_count, depth), jnp.float32),
            pltpu.VMEM((cells_x * cells_y, depth), jnp.float32),
        ],
        name="step",
    )(potential, recovery, fiber_angles, down, up, low, high, row, deep, wide)


def solution(mesh):
    placed = (
        P("gx", "gy", None),
        P("gx", "gy", None),
        P(None, "gx", "gy", None),
        P(None, ("gx", "gy")),
        P("gx", "gy", None),
    )
    return jax.shard_map(
        local,
        mesh=mesh,
        in_specs=placed,
        out_specs=(P("gx", "gy", None), P("gx", "gy", None)),
        check_vma=False,
    )
```

```python
import functools

import jax
import jax.numpy as jnp
import numpy as np
from jax import lax
from jax.experimental import pallas as pl
from jax.experimental.pallas import tpu as pltpu
from jax.sharding import PartitionSpec as P

RATIO = 4
SAME, EVEN, ODD = 0, 1, 2

sigma_fiber = 1.0
sigma_cross = 0.3
time_step = 0.1
excite_gain = 8.0
excite_level = 0.15
stretch_gain = 10.0
stretch_reversal = 0.6
recover_rate = 0.5


def round_up(value, multiple):
    return -(-value // multiple) * multiple


def interpolation(count):
    weights = np.zeros((RATIO * count + 2, count + 2))
    for cell in range(-1, RATIO * count + 1):
        element, position = cell // RATIO, cell % RATIO
        offset = (position + 0.5) / RATIO - 0.5
        weights[cell + 1, element + 1] += 1.0 - abs(offset)
        weights[cell + 1, element + 1 + (1 if offset > 0 else -1)] += abs(offset)
    return weights


def fit_series():
    nodes = np.cos((np.arange(64) + 0.5) * np.pi / 64)
    square = (nodes + 1.0) * 0.5 * np.pi**2
    root = np.sqrt(square)
    series = []
    for values in (np.sin(root) / root, np.cos(root)):
        fitted = np.polynomial.chebyshev.Chebyshev.fit(square, values, 8, domain=[0.0, np.pi**2])
        series.append(fitted.convert(kind=np.polynomial.Polynomial).coef)
    return series


SINE, COSINE = fit_series()


def horner(series, square):
    total = jnp.full_like(square, float(series[-1]))
    for coefficient in series[-2::-1]:
        total = total * square + float(coefficient)
    return total


def sine_cosine(angle):
    square = angle * angle
    return (angle * horner(SINE, square), horner(COSINE, square))


def parts_of(values, count):
    pieces = []
    for _ in range(count):
        piece = values.astype(jnp.bfloat16)
        pieces.append(piece)
        values = values - piece.astype(jnp.float32)
    return pieces


def dot(left, right):
    return jnp.dot(left, right, preferred_element_type=jnp.float32)


def pack(potential_ref, angle_ref, deform_ref, slot_ref, *out_refs, keys, rows):
    cells_x, cells_y = potential_ref.shape[:2]
    components, held = deform_ref.shape
    columns, coarse_depth = slot_ref.shape[1:]
    gx = lax.axis_index("gx")
    gy = lax.axis_index("gy")
    for key, out_ref in zip(keys, out_refs):
        kind, flips = key
        goes_up = (gx % 2 == 0) if kind == EVEN else (gx % 2 == 1)
        goes_right = (gy ^ flips) > gy
        depth = out_ref.shape[1]
        start = out_ref.shape[0] - rows
        out_ref[start:, :] = jnp.zeros((rows, depth), jnp.float32)
        out_ref[start : start + components, 0:held] = deform_ref[...]
        out_ref[start + components : start + components + columns, 0:coarse_depth] = slot_ref[
            0
        ].astype(jnp.float32)
        if kind == SAME:
            if start:
                out_ref[0:start, :] = jnp.zeros((start, depth), jnp.float32)
                for x in range(cells_x):
                    for line, source in (
                        (x, potential_ref.at[x]),
                        (cells_x + x, angle_ref.at[0, x]),
                        (2 * cells_x + x, angle_ref.at[1, x]),
                    ):
                        out_ref[line : line + 1] = jnp.where(
                            goes_right, source[cells_y - 1 : cells_y], source[0:1]
                        )
        elif flips == 0:
            out_ref[0:cells_y] = jnp.where(goes_up, potential_ref[cells_x - 1], potential_ref[0])
            for number in range(2):
                first = (number + 1) * cells_y
                out_ref[first : first + cells_y] = jnp.where(
                    goes_up, angle_ref[number, cells_x - 1], angle_ref[number, 0]
                )
        else:
            corner = start + components + columns
            above = jnp.where(
                goes_right, potential_ref[cells_x - 1, cells_y - 1 :], potential_ref[cells_x - 1, 0:1]
            )
            below = jnp.where(
                goes_right, potential_ref[0, cells_y - 1 :], potential_ref[0, 0:1]
            )
            out_ref[corner : corner + 1] = jnp.where(goes_up, above, below)


def tensors(entries, azimuth, elevation):
    sin_u, cos_u = sine_cosine(azimuth)
    sin_e, cos_e = sine_cosine(elevation)
    fiber = [cos_u * cos_e, sin_u * cos_e, sin_e]

    def element(row_index, col_index):
        return entries[3 * (row_index % 3) + col_index % 3]

    cofactor = [
        [
            element(row + 1, col + 1) * element(row + 2, col + 2)
            - element(row + 1, col + 2) * element(row + 2, col + 1)
            for col in range(3)
        ]
        for row in range(3)
    ]
    determinant = (
        element(0, 0) * cofactor[0][0]
        + element(0, 1) * cofactor[0][1]
        + element(0, 2) * cofactor[0][2]
    )
    scale = 1.0 / determinant
    adjugate = [[cofactor[col][row] for col in range(3)] for row in range(3)]
    pulled = [
        adjugate[row][0] * fiber[0] + adjugate[row][1] * fiber[1] + adjugate[row][2] * fiber[2]
        for row in range(3)
    ]
    cross = (scale * scale) * sigma_cross
    along = (scale * scale) * (sigma_fiber - sigma_cross)
    conduct = []
    for first, second in ((0, 0), (1, 1), (2, 2), (0, 1), (0, 2), (1, 2)):
        metric = (
            adjugate[first][0] * adjugate[second][0]
            + adjugate[first][1] * adjugate[second][1]
            + adjugate[first][2] * adjugate[second][2]
        )
        conduct.append(cross * metric + along * (pulled[first] * pulled[second]))
    return conduct, fiber


def stretch_of(entries, fiber):
    total = None
    for row in range(3):
        value = (
            entries[3 * row] * fiber[0]
            + entries[3 * row + 1] * fiber[1]
            + entries[3 * row + 2] * fiber[2]
        )
        total = value * value if total is None else total + value * value
    return jnp.sqrt(total)


def step(
    potential_ref,
    recovery_ref,
    angle_ref,
    deform_ref,
    slot_ref,
    deep_ref,
    wide_ref,
    *refs,
    keys,
    rows,
):
    packets = dict(zip(keys, refs))
    (
        potential_out,
        recovery_out,
        table_ref,
        low_ref,
        high_ref,
        coarse_ref,
        fine_ref,
        conduct_ref,
        stretch_ref,
    ) = refs[len(keys) :]
    cells_x, cells_y, depth = potential_ref.shape
    components, held = deform_ref.shape
    elements, columns, coarse_depth = slot_ref.shape
    devices = lax.axis_size("gy")
    gx = lax.axis_index("gx")
    gy = lax.axis_index("gy")
    at_first_x = gx == 0
    at_last_x = gx == lax.axis_size("gx") - 1
    at_first_y = gy == 0
    at_last_y = gy == devices - 1
    is_odd = gx % 2 == 1
    rims = [flips for flips in range(1, devices) if flips & (flips + 1) == 0]

    def beside(values, towards, own):
        chosen = own
        for flips, value in values.items():
            chosen = jnp.where((gy ^ flips) == towards, value, chosen)
        return chosen

    table_ref[1, 0] = jnp.zeros((rows, held), jnp.float32)
    table_ref[1, 0, 0:components] = deform_ref[...]
    table_ref[1, 0, components : components + columns, 0:coarse_depth] = slot_ref[0].astype(
        jnp.float32
    )
    for flips in range(devices):
        if flips:
            table_ref[1, flips] = packets[SAME, flips][-rows:, :]
        own = table_ref[1, flips]
        even = packets[EVEN, flips][-rows:, :]
        odd = packets[ODD, flips][-rows:, :]
        table_ref[0, flips] = jnp.where(at_first_x, own, jnp.where(is_odd, even, odd))
        table_ref[2, flips] = jnp.where(at_last_x, own, jnp.where(is_odd, odd, even))
    even_ref, odd_ref = packets[EVEN, 0], packets[ODD, 0]
    for number in range(3):
        first = number * cells_y
        own = (potential_ref, angle_ref.at[0], angle_ref.at[1])[number]
        even = even_ref[first : first + cells_y]
        odd = odd_ref[first : first + cells_y]
        low_ref[first : first + cells_y] = jnp.where(
            at_first_x, own[0], jnp.where(is_odd, even, odd)
        )
        high_ref[first : first + cells_y] = jnp.where(
            at_last_x, own[cells_x - 1], jnp.where(is_odd, odd, even)
        )
    corner = components + columns
    rim_rows = []
    for side, towards in ((0, gy - 1), (cells_y - 1, gy + 1)):
        inner = [
            beside(
                {f: packets[SAME, f][x : x + 1] for f in rims},
                towards,
                potential_ref[x, side : side + 1],
            )
            for x in range(cells_x)
        ]
        ends = []
        for row, edge_ref, at_edge, near in (
            (0, low_ref, at_first_x, inner[0]),
            (2, high_ref, at_last_x, inner[-1]),
        ):
            value = beside(
                {f: table_ref[row, f, corner : corner + 1] for f in rims},
                towards,
                edge_ref[side : side + 1],
            )
            ends.append(jnp.where(at_edge, near, value))
        filler = [jnp.zeros_like(inner[0])] * (round_up(cells_x + 2, 8) - cells_x - 2)
        rim_rows.append(jnp.concatenate([ends[0]] + inner + [ends[1]] + filler, axis=0))
    rim_low, rim_high = rim_rows

    lanes = 2 * coarse_depth
    lane = lax.broadcasted_iota(jnp.int32, (1, lanes), 1)
    count = columns + 2
    gathered = [[None] * (count // 2) for _ in range(elements + 2)]
    for r in range(elements + 2):
        own = table_ref[r, 0, components : components + columns, 0:lanes]
        last = components + columns - 1
        before = beside(
            {f: table_ref[r, f, last : last + 1, 0:lanes] for f in rims}, gy - 1, own[0:1]
        )
        after = beside(
            {f: table_ref[r, f, components : components + 1, 0:lanes] for f in rims},
            gy + 1,
            own[columns - 1 : columns],
        )
        line = [before] + [own[c : c + 1] for c in range(columns)] + [after]
        table_parts = parts_of(table_ref[r].reshape(devices * rows, held), 3)
        for pair in range(count // 2):
            slots = jnp.where(
                lane < coarse_depth,
                line[2 * pair],
                pltpu.roll(line[2 * pair + 1], coarse_depth, 1),
            ).astype(jnp.int32)
            place = slots % held
            flips_of = ((slots // held) % devices) ^ gy
            match = lax.broadcasted_iota(jnp.int32, (held, lanes), 0) == place
            chosen = jnp.where(match, 1.0, 0.0).astype(jnp.bfloat16)
            values = dot(table_parts[0], chosen)
            for part in table_parts[1:]:
                values = values + dot(part, chosen)
            picked = values[0:rows]
            for flips in range(1, devices):
                picked = jnp.where(
                    flips_of == flips, values[flips * rows : (flips + 1) * rows], picked
                )
            gathered[r][pair] = picked

    tall = (elements + 2) * rows
    for pair in range(count // 2):
        stacked = jnp.concatenate([gathered[r][pair] for r in range(elements + 2)], axis=0)
        values = None
        for part in parts_of(stacked, 3):
            term = dot(part, deep_ref[...])
            values = term if values is None else values + term
        coarse_ref[2 * pair * tall : (2 * pair + 1) * tall] = values[:, 0:depth]
        coarse_ref[(2 * pair + 1) * tall : (2 * pair + 2) * tall] = values[:, depth : 2 * depth]
    coarse_parts = parts_of(coarse_ref[...], 2)
    fine_ref[...] = dot(wide_ref[...], coarse_parts[0]) + dot(wide_ref[...], coarse_parts[1])

    total_rows = fine_ref.shape[0] // components
    inner_rows = cells_x * cells_y
    chunk = 8
    for start in range(0, total_rows, chunk):
        entries = [
            fine_ref[k * total_rows + start : k * total_rows + start + chunk]
            for k in range(components)
        ]
        if start < inner_rows:
            x, y = start // cells_y, start % cells_y
            azimuth = angle_ref[0, x, y : y + chunk]
            elevation = angle_ref[1, x, y : y + chunk]
        elif start < inner_rows + 2 * cells_y:
            edge_ref = low_ref if start < inner_rows + cells_y else high_ref
            y = (start - inner_rows) % cells_y
            azimuth = edge_ref[cells_y + y : cells_y + y + chunk]
            elevation = edge_ref[2 * cells_y + y : 2 * cells_y + y + chunk]
        else:
            pieces = [[], []]
            for number in range(2):
                first = (number + 1) * cells_x
                for towards in (gy - 1, gy + 1):
                    values = {f: packets[SAME, f][first : first + cells_x] for f in rims}
                    pieces[number].append(beside(values, towards, values[rims[0]]))
            azimuth = jnp.concatenate(pieces[0], axis=0)
            elevation = jnp.concatenate(pieces[1], axis=0)
        conduct, fiber = tensors(entries, azimuth, elevation)
        for number in range(6):
            conduct_ref[number, start : start + chunk] = conduct[number]
        if start < inner_rows:
            stretch_ref[start : start + chunk] = stretch_of(entries, fiber)

    row_index = lax.broadcasted_iota(jnp.int32, (cells_y, depth), 0)
    lane_index = lax.broadcasted_iota(jnp.int32, (cells_y, depth), 1)
    def deeper(values, first):
        return jnp.where(first, values, pltpu.roll(values, 1, 1))

    def grad_z(values):
        index = lax.broadcasted_iota(jnp.int32, values.shape, 1)
        after = jnp.where(index == depth - 1, values, pltpu.roll(values, depth - 1, 1))
        before = jnp.where(index == 0, values, pltpu.roll(values, 1, 1))
        return (after - before) * 0.5

    def lower_y(values, rim):
        return jnp.where(row_index == 0, rim, pltpu.roll(values, 1, 0))

    def upper_y(values, rim):
        return jnp.where(row_index == cells_y - 1, rim, pltpu.roll(values, cells_y - 1, 0))

    def voltage_at(x):
        if x < 0:
            return low_ref[0:cells_y]
        if x >= cells_x:
            return high_ref[0:cells_y]
        return potential_ref[x]

    def conduct_at(number, x):
        if x < 0:
            return conduct_ref[number, inner_rows : inner_rows + cells_y]
        if x >= cells_x:
            return conduct_ref[number, inner_rows + cells_y : inner_rows + 2 * cells_y]
        return conduct_ref[number, x * cells_y : (x + 1) * cells_y]

    voltages = [voltage_at(x) for x in range(-1, cells_x + 1)]
    grads_y = [
        (
            upper_y(voltages[x], rim_high[x : x + 1])
            - lower_y(voltages[x], rim_low[x : x + 1])
        )
        * 0.5
        for x in range(cells_x + 2)
    ]
    grads_z = [grad_z(values) for values in voltages]
    rim_z = [grad_z(rim_low), grad_z(rim_high)]

    def flux(tensor_a, tensor_b, grads_a, grads_b, straight, voltage_a, voltage_b):
        total = None
        for place in range(3):
            mean = (tensor_a[place] + tensor_b[place]) * 0.5
            if place == straight:
                term = mean * (voltage_b - voltage_a)
            else:
                term = mean * ((grads_a[place] + grads_b[place]) * 0.5)
            total = term if total is None else total + term
        return total

    flux_x = []
    for face in range(cells_x + 1):
        value = flux(
            [conduct_at(n, face - 1) for n in (0, 3, 4)],
            [conduct_at(n, face) for n in (0, 3, 4)],
            [None, grads_y[face], grads_z[face]],
            [None, grads_y[face + 1], grads_z[face + 1]],
            0,
            voltages[face],
            voltages[face + 1],
        )
        if face == 0:
            value = jnp.where(at_first_x, 0.0, value)
        if face == cells_x:
            value = jnp.where(at_last_x, 0.0, value)
        flux_x.append(value)

    rim_start = inner_rows + 2 * cells_y
    for x in range(cells_x):
        voltage = voltages[x + 1]
        grad_x = (voltages[x + 2] - voltages[x]) * 0.5
        grad_y = grads_y[x + 1]
        grad_zz = grads_z[x + 1]
        tensor = [conduct_at(n, x) for n in (3, 1, 5)]
        low_tensor = [conduct_ref[n, rim_start + x : rim_start + x + 1] for n in (3, 1, 5)]
        high_tensor = [
            conduct_ref[n, rim_start + cells_x + x : rim_start + cells_x + x + 1]
            for n in (3, 1, 5)
        ]
        low_grads = [
            (rim_low[x + 2 : x + 3] - rim_low[x : x + 1]) * 0.5,
            None,
            rim_z[0][x + 1 : x + 2],
        ]
        high_grads = [
            (rim_high[x + 2 : x + 3] - rim_high[x : x + 1]) * 0.5,
            None,
            rim_z[1][x + 1 : x + 2],
        ]
        lower = flux(
            [lower_y(tensor[n], low_tensor[n]) for n in range(3)],
            tensor,
            [lower_y(grad_x, low_grads[0]), None, lower_y(grad_zz, low_grads[2])],
            [grad_x, None, grad_zz],
            1,
            lower_y(voltage, rim_low[x + 1 : x + 2]),
            voltage,
        )
        lower = jnp.where((row_index == 0) & at_first_y, 0.0, lower)
        top = flux(
            [value[cells_y - 1 : cells_y] for value in tensor],
            high_tensor,
            [grad_x[cells_y - 1 : cells_y], None, grad_zz[cells_y - 1 : cells_y]],
            high_grads,
            1,
            voltage[cells_y - 1 : cells_y],
            rim_high[x + 1 : x + 2],
        )
        top = jnp.where(at_last_y, 0.0, top)
        divergent = flux_x[x + 1] - flux_x[x] + (upper_y(lower, top) - lower)
        first = lane_index == 0
        tensor = [conduct_at(n, x) for n in (4, 5, 2)]
        before = flux(
            [deeper(value, first) for value in tensor],
            tensor,
            [deeper(grad_x, first), deeper(grad_y, first), None],
            [grad_x, grad_y, None],
            2,
            deeper(voltage, first),
            voltage,
        )
        before = jnp.where(first, 0.0, before)
        divergent = divergent + (pltpu.roll(before, depth - 1, 1) - before)
        recovery = recovery_ref[x]
        stretch = stretch_ref[x * cells_y : (x + 1) * cells_y]
        current = (
            excite_gain * voltage * (voltage - excite_level) * (voltage - 1.0)
            + voltage * recovery
        )
        current = current + stretch_gain * jnp.maximum(stretch - 1.0, 0.0) * (
            voltage - stretch_reversal
        )
        potential_out[x] = voltage + time_step * (divergent - current)
        recovery_out[x] = recovery + time_step * recover_rate * (
            -recovery - excite_gain * voltage * (voltage - excite_level - 1.0)
        )


def weights_of(cells_x, cells_y, columns, coarse_depth, depth, rows, components):
    elements = cells_x // RATIO
    deep = np.zeros((coarse_depth, depth))
    along_z = interpolation(coarse_depth)[1:-1]
    deep += along_z[:, 1:-1].T
    deep[0] += along_z[:, 0]
    deep[-1] += along_z[:, -1]
    pair = np.zeros((2 * coarse_depth, 2 * depth))
    pair[:coarse_depth, :depth] = deep
    pair[coarse_depth:, depth:] = deep
    along_x = interpolation(elements)
    along_y = interpolation(columns)
    places = [(x + 1, y + 1) for x in range(cells_x) for y in range(cells_y)]
    places += [(x, y + 1) for x in (0, cells_x + 1) for y in range(cells_y)]
    places += [(x + 1, y) for y in (0, cells_y + 1) for x in range(cells_x)]
    wide = np.zeros((components, len(places), columns + 2, elements + 2, rows))
    for line, (x, y) in enumerate(places):
        block = along_y[y][:, None] * along_x[x][None, :]
        for k in range(components):
            wide[k, line, :, :, k] = block
    wide = wide.reshape(components * len(places), -1)
    return jnp.asarray(pair, jnp.bfloat16), jnp.asarray(wide, jnp.bfloat16), len(places)


def local(potential, recovery, fiber_angles, deform, elem_slot):
    cells_x, cells_y, depth = potential.shape
    elements, columns, coarse_depth = elem_slot.shape
    components, held = deform.shape
    rows = round_up(components + columns + 1, 8)
    deep, wide, line_count = weights_of(
        cells_x, cells_y, columns, coarse_depth, depth, rows, components
    )
    across, down = lax.axis_size("gx"), lax.axis_size("gy")
    assert elements == 1 and columns % 2 == 0 and held == depth
    assert down & (down - 1) == 0 and down > 1 and rows > components + columns

    keys = [(kind, flips) for kind in (EVEN, ODD, SAME) for flips in range(down)]
    keys.remove((SAME, 0))

    def is_rim(flips):
        return flips and flips & (flips + 1) == 0

    def sender(key):
        return key if key[1] == 0 or is_rim(key[1]) else None

    senders = [key for key in keys if sender(key)] + [None]
    shapes = []
    for key in senders:
        extra = 0
        if key is not None and key[0] == SAME:
            extra = round_up(3 * cells_x, 8)
        elif key is not None and key[1] == 0:
            extra = 3 * cells_y
        shapes.append(jax.ShapeDtypeStruct((extra + rows, depth), jnp.float32))
    packed = pl.pallas_call(
        functools.partial(
            pack, keys=[(SAME, 0) if key is None else key for key in senders], rows=rows
        ),
        out_shape=shapes,
        name="pack",
    )(potential, fiber_angles, deform, elem_slot)
    packed = dict(zip(senders, packed))

    def pairs(kind, flips):
        for x in range(across):
            peer = x if kind == SAME else (x ^ 1 if kind == EVEN else ((x + 1) ^ 1) - 1)
            if 0 <= peer < across:
                for y in range(down):
                    yield (x * down + y, peer * down + (y ^ flips))

    got = [lax.ppermute(packed[sender(key)], ("gx", "gy"), list(pairs(*key))) for key in keys]
    block = jax.ShapeDtypeStruct((cells_x, cells_y, depth), jnp.float32)
    return pl.pallas_call(
        functools.partial(step, keys=keys, rows=rows),
        out_shape=(block, block),
        scratch_shapes=[
            pltpu.VMEM((elements + 2, down, rows, held), jnp.float32),
            pltpu.VMEM((3 * cells_y, depth), jnp.float32),
            pltpu.VMEM((3 * cells_y, depth), jnp.float32),
            pltpu.VMEM(((columns + 2) * (elements + 2) * rows, depth), jnp.float32),
            pltpu.VMEM((components * line_count, depth), jnp.float32),
            pltpu.VMEM((6, line_count, depth), jnp.float32),
            pltpu.VMEM((cells_x * cells_y, depth), jnp.float32),
        ],
        name="step",
    )(potential, recovery, fiber_angles, deform, elem_slot, deep, wide, *got)


def solution(mesh):
    placed = (
        P("gx", "gy", None),
        P("gx", "gy", None),
        P(None, "gx", "gy", None),
        P(None, ("gx", "gy")),
        P("gx", "gy", None),
    )
    return jax.shard_map(
        local,
        mesh=mesh,
        in_specs=placed,
        out_specs=(P("gx", "gy", None), P("gx", "gy", None)),
        check_vma=False,
    )
```

```python
import functools

import jax
import jax.numpy as jnp
import numpy as np
from jax import lax
from jax.experimental import pallas as pl
from jax.experimental.pallas import tpu as pltpu
from jax.sharding import PartitionSpec as P

RATIO = 4

sigma_fiber = 1.0
sigma_cross = 0.3
time_step = 0.1
excite_gain = 8.0
excite_level = 0.15
stretch_gain = 10.0
stretch_reversal = 0.6
recover_rate = 0.5


def IN(values):
    return pltpu.with_memory_space_constraint(values, pltpu.VMEM)


def OUT(shape):
    return pltpu.VMEM(shape, jnp.float32)


def round_up(value, multiple):
    return -(-value // multiple) * multiple


def interpolation(count):
    weights = np.zeros((RATIO * count + 2, count + 2))
    for cell in range(-1, RATIO * count + 1):
        element, position = cell // RATIO, cell % RATIO
        offset = (position + 0.5) / RATIO - 0.5
        weights[cell + 1, element + 1] += 1.0 - abs(offset)
        weights[cell + 1, element + 1 + (1 if offset > 0 else -1)] += abs(offset)
    return weights


def fit_series():
    nodes = np.cos((np.arange(64) + 0.5) * np.pi / 64)
    square = (nodes + 1.0) * 0.5 * np.pi**2
    root = np.sqrt(square)
    series = []
    for values in (np.sin(root) / root, np.cos(root)):
        fitted = np.polynomial.chebyshev.Chebyshev.fit(square, values, 8, domain=[0.0, np.pi**2])
        series.append(fitted.convert(kind=np.polynomial.Polynomial).coef)
    return series


SINE, COSINE = fit_series()


def horner(series, square):
    total = jnp.full_like(square, float(series[-1]))
    for coefficient in series[-2::-1]:
        total = total * square + float(coefficient)
    return total


def sine_cosine(angle):
    square = angle * angle
    return (angle * horner(SINE, square), horner(COSINE, square))


def parts_of(values, count):
    pieces = []
    for _ in range(count):
        piece = values.astype(jnp.bfloat16)
        pieces.append(piece)
        values = values - piece.astype(jnp.float32)
    return pieces


def dot(left, right):
    return jnp.dot(left, right, preferred_element_type=jnp.float32)


def fill_gradients(out_ref, start, deform_ref, slot_ref, rows):
    components, held = deform_ref.shape
    columns, coarse_depth = slot_ref.shape[1:]
    out_ref[start : start + rows, :] = jnp.zeros((rows, out_ref.shape[1]), jnp.float32)
    out_ref[start : start + components, 0:held] = deform_ref[...]
    out_ref[start + components : start + components + columns, 0:coarse_depth] = slot_ref[
        0
    ].astype(jnp.float32)


def pack_x(potential_ref, angle_ref, deform_ref, slot_ref, even_ref, odd_ref, *, rows):
    cells_x, cells_y = potential_ref.shape[:2]
    gx = lax.axis_index("gx")
    for out_ref, goes_up in ((even_ref, gx % 2 == 0), (odd_ref, gx % 2 == 1)):
        sources = (potential_ref, angle_ref.at[0], angle_ref.at[1])
        for number, source in enumerate(sources):
            out_ref[number * cells_y : (number + 1) * cells_y] = jnp.where(
                goes_up, source[cells_x - 1], source[0]
            )
        fill_gradients(out_ref, 3 * cells_y, deform_ref, slot_ref, rows)


def pack_y(
    potential_ref, angle_ref, deform_ref, slot_ref, even_ref, odd_ref, *out_refs, rims, rows
):
    low_ref, high_ref, row_ref = out_refs[:3]
    cells_x, cells_y, depth = potential_ref.shape
    gx = lax.axis_index("gx")
    gy = lax.axis_index("gy")
    at_first = gx == 0
    at_last = gx == lax.axis_size("gx") - 1
    is_odd = gx % 2 == 1
    fill_gradients(row_ref, rows, deform_ref, slot_ref, rows)
    even, odd = even_ref[3 * cells_y :], odd_ref[3 * cells_y :]
    own = row_ref[rows : 2 * rows]
    row_ref[0:rows] = jnp.where(at_first, own, jnp.where(is_odd, even, odd))
    row_ref[2 * rows :] = jnp.where(at_last, own, jnp.where(is_odd, odd, even))
    for number, source in enumerate((potential_ref, angle_ref.at[0], angle_ref.at[1])):
        part = slice(number * cells_y, (number + 1) * cells_y)
        even, odd = even_ref[part], odd_ref[part]
        low_ref[part] = jnp.where(at_first, source[0], jnp.where(is_odd, even, odd))
        high_ref[part] = jnp.where(at_last, source[cells_x - 1], jnp.where(is_odd, odd, even))
    first_rows = round_up(cells_x + 2, 8)
    for flips, out_ref in zip(rims, out_refs[3:]):
        goes_right = (gy ^ flips) > gy
        start = out_ref.shape[0] - 3 * rows
        out_ref[start:] = row_ref[...]
        out_ref[0:start] = jnp.zeros((start, depth), jnp.float32)
        lines = [(0, low_ref), (1 + cells_x, high_ref)]
        for x in range(cells_x):
            lines.append((1 + x, potential_ref.at[x]))
            lines.append((first_rows + x, angle_ref.at[0, x]))
            lines.append((first_rows + cells_x + x, angle_ref.at[1, x]))
        for line, source in lines:
            out_ref[line : line + 1] = jnp.where(
                goes_right, source[cells_y - 1 : cells_y], source[0:1]
            )


def tensors(entries, azimuth, elevation):
    sin_u, cos_u = sine_cosine(azimuth)
    sin_e, cos_e = sine_cosine(elevation)
    fiber = [cos_u * cos_e, sin_u * cos_e, sin_e]

    def element(row_index, col_index):
        return entries[3 * (row_index % 3) + col_index % 3]

    cofactor = [
        [
            element(row + 1, col + 1) * element(row + 2, col + 2)
            - element(row + 1, col + 2) * element(row + 2, col + 1)
            for col in range(3)
        ]
        for row in range(3)
    ]
    determinant = (
        element(0, 0) * cofactor[0][0]
        + element(0, 1) * cofactor[0][1]
        + element(0, 2) * cofactor[0][2]
    )
    scale = 1.0 / determinant
    adjugate = [[cofactor[col][row] for col in range(3)] for row in range(3)]
    pulled = [
        adjugate[row][0] * fiber[0] + adjugate[row][1] * fiber[1] + adjugate[row][2] * fiber[2]
        for row in range(3)
    ]
    cross = (scale * scale) * sigma_cross
    along = (scale * scale) * (sigma_fiber - sigma_cross)
    conduct = []
    for first, second in ((0, 0), (1, 1), (2, 2), (0, 1), (0, 2), (1, 2)):
        metric = (
            adjugate[first][0] * adjugate[second][0]
            + adjugate[first][1] * adjugate[second][1]
            + adjugate[first][2] * adjugate[second][2]
        )
        conduct.append(cross * metric + along * (pulled[first] * pulled[second]))
    return conduct, fiber


def stretch_of(entries, fiber):
    total = None
    for row in range(3):
        value = (
            entries[3 * row] * fiber[0]
            + entries[3 * row + 1] * fiber[1]
            + entries[3 * row + 2] * fiber[2]
        )
        total = value * value if total is None else total + value * value
    return jnp.sqrt(total)


def step(
    potential_ref,
    recovery_ref,
    angle_ref,
    low_ref,
    high_ref,
    line_ref,
    side_ref,
    deep_ref,
    *refs,
    components,
    held,
    columns,
    coarse_depth,
    rows,
    devices,
):
    packets = refs[:devices]
    (
        potential_out,
        recovery_out,
        coarse_ref,
        fine_ref,
        conduct_ref,
        stretch_ref,
    ) = refs[devices:]
    cells_x, cells_y, depth = potential_ref.shape
    elements = cells_x // RATIO
    gx = lax.axis_index("gx")
    gy = lax.axis_index("gy")
    at_first_x = gx == 0
    at_last_x = gx == lax.axis_size("gx") - 1
    at_first_y = gy == 0
    at_last_y = gy == devices - 1
    rims = [flips for flips in range(1, devices) if is_rim(flips)]

    def beside(values, towards, own):
        chosen = own
        for flips, value in values.items():
            chosen = jnp.where((gy ^ flips) == towards, value, chosen)
        return chosen

    def table(r, flips):
        start = packets[flips].shape[0] - (elements + 2 - r) * rows
        return packets[flips].at[start : start + rows]

    first_rows = round_up(cells_x + 2, 8)
    rim_rows = []
    for side, towards in ((0, gy - 1), (cells_y - 1, gy + 1)):
        sources = [low_ref] + [potential_ref.at[x] for x in range(cells_x)] + [high_ref]
        own = [source[side : side + 1] for source in sources]
        own += [jnp.zeros_like(own[0])] * (first_rows - len(own))
        values = {flips: packets[flips][0:first_rows] for flips in rims}
        rim_rows.append(beside(values, towards, jnp.concatenate(own, axis=0)))
    rim_low, rim_high = rim_rows

    lanes = 2 * coarse_depth
    lane = lax.broadcasted_iota(jnp.int32, (1, lanes), 1)
    count = columns + 2
    gathered = [[None] * (count // 2) for _ in range(elements + 2)]
    for r in range(elements + 2):
        own = table(r, 0)[components : components + columns, 0:lanes]
        last = components + columns - 1
        before = beside(
            {f: table(r, f)[last : last + 1, 0:lanes] for f in rims}, gy - 1, own[0:1]
        )
        after = beside(
            {f: table(r, f)[components : components + 1, 0:lanes] for f in rims},
            gy + 1,
            own[columns - 1 : columns],
        )
        line = [before] + [own[c : c + 1] for c in range(columns)] + [after]
        table_parts = parts_of(
            jnp.concatenate([table(r, f)[:, 0:held] for f in range(devices)], axis=0), 3
        )
        for pair in range(count // 2):
            slots = jnp.where(
                lane < coarse_depth,
                line[2 * pair],
                pltpu.roll(line[2 * pair + 1], coarse_depth, 1),
            ).astype(jnp.int32)
            place = slots % held
            flips_of = ((slots // held) % devices) ^ gy
            match = lax.broadcasted_iota(jnp.int32, (held, lanes), 0) == place
            chosen = jnp.where(match, 1.0, 0.0).astype(jnp.bfloat16)
            values = dot(table_parts[0], chosen)
            for part in table_parts[1:]:
                values = values + dot(part, chosen)
            picked = values[0:rows]
            for flips in range(1, devices):
                picked = jnp.where(
                    flips_of == flips, values[flips * rows : (flips + 1) * rows], picked
                )
            gathered[r][pair] = picked

    tall = (elements + 2) * rows
    for pair in range(count // 2):
        stacked = jnp.concatenate([gathered[r][pair] for r in range(elements + 2)], axis=0)
        values = None
        for part in parts_of(stacked, 3):
            term = dot(part, deep_ref[...])
            values = term if values is None else values + term
        coarse_ref[2 * pair * tall : (2 * pair + 1) * tall] = values[:, 0:depth]
        coarse_ref[(2 * pair + 1) * tall : (2 * pair + 2) * tall] = values[:, depth : 2 * depth]
    block_rows = cells_y * components
    along_x = interpolation(elements)
    blended = []
    for x in range(cells_x + 2):
        columns_x = []
        for c in range(count):
            total = None
            for r in range(elements + 2):
                weight = float(along_x[x, r])
                if weight:
                    start = c * tall + r * rows
                    term = weight * coarse_ref[start : start + rows]
                    total = term if total is None else total + term
            columns_x.append(total)
        pieces = parts_of(jnp.concatenate(columns_x, axis=0), 2)
        blended.append(pieces)
        place = x - 1 if 0 < x <= cells_x else (cells_x if x == 0 else cells_x + 1)
        fine_ref[place * block_rows : (place + 1) * block_rows] = dot(
            line_ref[...], pieces[0]
        ) + dot(line_ref[...], pieces[1])
    side_base = (cells_x + 2) * block_rows
    total = None
    for number in range(2):
        stacked = jnp.concatenate([blended[x + 1][number] for x in range(cells_x)], axis=0)
        term = dot(side_ref[...], stacked)
        total = term if total is None else total + term
    fine_ref[side_base:] = total

    total_rows = fine_ref.shape[0] // components
    inner_rows = cells_x * cells_y
    chunk = 8
    for start in range(0, total_rows, chunk):
        if start < inner_rows + 2 * cells_y:
            base, stride = start // cells_y * block_rows + start % cells_y, cells_y
        else:
            base, stride = side_base, total_rows - inner_rows - 2 * cells_y
        entries = [
            fine_ref[base + k * stride : base + k * stride + chunk] for k in range(components)
        ]
        if start < inner_rows:
            x, y = start // cells_y, start % cells_y
            azimuth = angle_ref[0, x, y : y + chunk]
            elevation = angle_ref[1, x, y : y + chunk]
        elif start < inner_rows + 2 * cells_y:
            edge_ref = low_ref if start < inner_rows + cells_y else high_ref
            y = (start - inner_rows) % cells_y
            azimuth = edge_ref[cells_y + y : cells_y + y + chunk]
            elevation = edge_ref[2 * cells_y + y : 2 * cells_y + y + chunk]
        else:
            pieces = [[], []]
            for number in range(2):
                first = first_rows + number * cells_x
                for towards in (gy - 1, gy + 1):
                    values = {f: packets[f][first : first + cells_x] for f in rims}
                    pieces[number].append(beside(values, towards, values[rims[0]]))
            azimuth = jnp.concatenate(pieces[0], axis=0)
            elevation = jnp.concatenate(pieces[1], axis=0)
        conduct, fiber = tensors(entries, azimuth, elevation)
        for number in range(6):
            conduct_ref[number, start : start + chunk] = conduct[number]
        if start < inner_rows:
            stretch_ref[start : start + chunk] = stretch_of(entries, fiber)

    row_index = lax.broadcasted_iota(jnp.int32, (cells_y, depth), 0)
    lane_index = lax.broadcasted_iota(jnp.int32, (cells_y, depth), 1)
    def deeper(values, first):
        return jnp.where(first, values, pltpu.roll(values, 1, 1))

    def grad_z(values):
        index = lax.broadcasted_iota(jnp.int32, values.shape, 1)
        after = jnp.where(index == depth - 1, values, pltpu.roll(values, depth - 1, 1))
        before = jnp.where(index == 0, values, pltpu.roll(values, 1, 1))
        return (after - before) * 0.5

    def lower_y(values, rim):
        return jnp.where(row_index == 0, rim, pltpu.roll(values, 1, 0))

    def upper_y(values, rim):
        return jnp.where(row_index == cells_y - 1, rim, pltpu.roll(values, cells_y - 1, 0))

    def voltage_at(x):
        if x < 0:
            return low_ref[0:cells_y]
        if x >= cells_x:
            return high_ref[0:cells_y]
        return potential_ref[x]

    def conduct_at(number, x):
        if x < 0:
            return conduct_ref[number, inner_rows : inner_rows + cells_y]
        if x >= cells_x:
            return conduct_ref[number, inner_rows + cells_y : inner_rows + 2 * cells_y]
        return conduct_ref[number, x * cells_y : (x + 1) * cells_y]

    voltages = [voltage_at(x) for x in range(-1, cells_x + 1)]
    grads_y = [
        (
            upper_y(voltages[x], rim_high[x : x + 1])
            - lower_y(voltages[x], rim_low[x : x + 1])
        )
        * 0.5
        for x in range(cells_x + 2)
    ]
    grads_z = [grad_z(values) for values in voltages]
    rim_z = [grad_z(rim_low), grad_z(rim_high)]

    def flux(tensor_a, tensor_b, grads_a, grads_b, straight, voltage_a, voltage_b):
        total = None
        for place in range(3):
            mean = (tensor_a[place] + tensor_b[place]) * 0.5
            if place == straight:
                term = mean * (voltage_b - voltage_a)
            else:
                term = mean * ((grads_a[place] + grads_b[place]) * 0.5)
            total = term if total is None else total + term
        return total

    flux_x = []
    for face in range(cells_x + 1):
        value = flux(
            [conduct_at(n, face - 1) for n in (0, 3, 4)],
            [conduct_at(n, face) for n in (0, 3, 4)],
            [None, grads_y[face], grads_z[face]],
            [None, grads_y[face + 1], grads_z[face + 1]],
            0,
            voltages[face],
            voltages[face + 1],
        )
        if face == 0:
            value = jnp.where(at_first_x, 0.0, value)
        if face == cells_x:
            value = jnp.where(at_last_x, 0.0, value)
        flux_x.append(value)

    rim_start = inner_rows + 2 * cells_y
    for x in range(cells_x):
        voltage = voltages[x + 1]
        grad_x = (voltages[x + 2] - voltages[x]) * 0.5
        grad_y = grads_y[x + 1]
        grad_zz = grads_z[x + 1]
        tensor = [conduct_at(n, x) for n in (3, 1, 5)]
        low_tensor = [conduct_ref[n, rim_start + x : rim_start + x + 1] for n in (3, 1, 5)]
        high_tensor = [
            conduct_ref[n, rim_start + cells_x + x : rim_start + cells_x + x + 1]
            for n in (3, 1, 5)
        ]
        low_grads = [
            (rim_low[x + 2 : x + 3] - rim_low[x : x + 1]) * 0.5,
            None,
            rim_z[0][x + 1 : x + 2],
        ]
        high_grads = [
            (rim_high[x + 2 : x + 3] - rim_high[x : x + 1]) * 0.5,
            None,
            rim_z[1][x + 1 : x + 2],
        ]
        lower = flux(
            [lower_y(tensor[n], low_tensor[n]) for n in range(3)],
            tensor,
            [lower_y(grad_x, low_grads[0]), None, lower_y(grad_zz, low_grads[2])],
            [grad_x, None, grad_zz],
            1,
            lower_y(voltage, rim_low[x + 1 : x + 2]),
            voltage,
        )
        lower = jnp.where((row_index == 0) & at_first_y, 0.0, lower)
        top = flux(
            [value[cells_y - 1 : cells_y] for value in tensor],
            high_tensor,
            [grad_x[cells_y - 1 : cells_y], None, grad_zz[cells_y - 1 : cells_y]],
            high_grads,
            1,
            voltage[cells_y - 1 : cells_y],
            rim_high[x + 1 : x + 2],
        )
        top = jnp.where(at_last_y, 0.0, top)
        divergent = flux_x[x + 1] - flux_x[x] + (upper_y(lower, top) - lower)
        first = lane_index == 0
        tensor = [conduct_at(n, x) for n in (4, 5, 2)]
        before = flux(
            [deeper(value, first) for value in tensor],
            tensor,
            [deeper(grad_x, first), deeper(grad_y, first), None],
            [grad_x, grad_y, None],
            2,
            deeper(voltage, first),
            voltage,
        )
        before = jnp.where(first, 0.0, before)
        divergent = divergent + (pltpu.roll(before, depth - 1, 1) - before)
        recovery = recovery_ref[x]
        stretch = stretch_ref[x * cells_y : (x + 1) * cells_y]
        current = (
            excite_gain * voltage * (voltage - excite_level) * (voltage - 1.0)
            + voltage * recovery
        )
        current = current + stretch_gain * jnp.maximum(stretch - 1.0, 0.0) * (
            voltage - stretch_reversal
        )
        potential_out[x] = voltage + time_step * (divergent - current)
        recovery_out[x] = recovery + time_step * recover_rate * (
            -recovery - excite_gain * voltage * (voltage - excite_level - 1.0)
        )


def weights_of(cells_x, cells_y, columns, coarse_depth, depth, rows, components):
    deep = np.zeros((coarse_depth, depth))
    along_z = interpolation(coarse_depth)[1:-1]
    deep += along_z[:, 1:-1].T
    deep[0] += along_z[:, 0]
    deep[-1] += along_z[:, -1]
    pair = np.zeros((2 * coarse_depth, 2 * depth))
    pair[:coarse_depth, :depth] = deep
    pair[coarse_depth:, depth:] = deep
    along_y = interpolation(columns)
    line = np.zeros((components, cells_y, columns + 2, rows))
    side = np.zeros((components, 2, cells_x, cells_x, columns + 2, rows))
    for k in range(components):
        line[k, :, :, k] = along_y[1:-1]
        for x in range(cells_x):
            side[k, 0, x, x, :, k] = along_y[0]
            side[k, 1, x, x, :, k] = along_y[-1]
    line = line.reshape(components * cells_y, -1)
    side = side.reshape(components * 2 * cells_x, -1)
    return [jnp.asarray(values, jnp.bfloat16) for values in (line, side, pair)]


def is_rim(flips):
    return flips > 0 and flips & (flips + 1) == 0


def local(potential, recovery, fiber_angles, deform, elem_slot):
    cells_x, cells_y, depth = potential.shape
    elements, columns, coarse_depth = elem_slot.shape
    components, held = deform.shape
    rows = round_up(components + columns + 1, 8)
    weights = weights_of(cells_x, cells_y, columns, coarse_depth, depth, rows, components)
    across, down = lax.axis_size("gx"), lax.axis_size("gy")
    assert elements == 1 and columns % 2 == 0 and held == depth
    assert down & (down - 1) == 0 and down > 1 and 2 * cells_x == 8

    def packet(count):
        return OUT((count, depth))

    arrays = (potential, fiber_angles, deform, elem_slot)
    even, odd = pl.pallas_call(
        functools.partial(pack_x, rows=rows),
        out_shape=[packet(3 * cells_y + rows)] * 2,
        name="pack_x",
    )(*arrays)
    even = lax.ppermute(even, "gx", [(x, x ^ 1) for x in range(across) if x ^ 1 < across])
    upward = [(x, x + 1) for x in range(1, across - 1, 2)]
    odd = lax.ppermute(odd, "gx", upward + [(high, low) for low, high in upward])
    rims = [flips for flips in range(1, down) if is_rim(flips)]
    side_rows = round_up(cells_x + 2, 8) + 2 * cells_x
    low, high, row, *sent = pl.pallas_call(
        functools.partial(pack_y, rims=rims, rows=rows),
        out_shape=[packet(3 * cells_y)] * 2
        + [packet(3 * rows)]
        + [packet(side_rows + 3 * rows)] * len(rims),
        name="pack_y",
    )(*arrays, IN(even), IN(odd))
    sent = dict(zip(rims, sent))
    packets = [IN(row)]
    for flips in range(1, down):
        pairs = [(y, y ^ flips) for y in range(down)]
        packets.append(IN(lax.ppermute(sent.get(flips, row), "gy", pairs)))
    block = jax.ShapeDtypeStruct((cells_x, cells_y, depth), jnp.float32)
    line_count = (cells_x + 2) * cells_y + 2 * cells_x
    return pl.pallas_call(
        functools.partial(
            step,
            components=components,
            held=held,
            columns=columns,
            coarse_depth=coarse_depth,
            rows=rows,
            devices=down,
        ),
        out_shape=(block, block),
        scratch_shapes=[
            pltpu.VMEM(((columns + 2) * (elements + 2) * rows, depth), jnp.float32),
            pltpu.VMEM((components * line_count, depth), jnp.float32),
            pltpu.VMEM((6, line_count, depth), jnp.float32),
            pltpu.VMEM((cells_x * cells_y, depth), jnp.float32),
        ],
        name="step",
    )(potential, recovery, fiber_angles, IN(low), IN(high), *weights, *packets)


def solution(mesh):
    placed = (
        P("gx", "gy", None),
        P("gx", "gy", None),
        P(None, "gx", "gy", None),
        P(None, ("gx", "gy")),
        P("gx", "gy", None),
    )
    return jax.shard_map(
        local,
        mesh=mesh,
        in_specs=placed,
        out_specs=(P("gx", "gy", None), P("gx", "gy", None)),
        check_vma=False,
    )
```

```python
import functools

import jax
import jax.numpy as jnp
import numpy as np
from jax import lax
from jax.experimental import pallas as pl
from jax.experimental.pallas import tpu as pltpu
from jax.sharding import PartitionSpec as P

RATIO = 4

sigma_fiber = 1.0
sigma_cross = 0.3
time_step = 0.1
excite_gain = 8.0
excite_level = 0.15
stretch_gain = 10.0
stretch_reversal = 0.6
recover_rate = 0.5


def IN(values):
    return pltpu.with_memory_space_constraint(values, pltpu.VMEM)


def OUT(shape):
    return pltpu.VMEM(shape, jnp.float32)


def round_up(value, multiple):
    return -(-value // multiple) * multiple


def interpolation(count):
    weights = np.zeros((RATIO * count + 2, count + 2))
    for cell in range(-1, RATIO * count + 1):
        element, position = cell // RATIO, cell % RATIO
        offset = (position + 0.5) / RATIO - 0.5
        weights[cell + 1, element + 1] += 1.0 - abs(offset)
        weights[cell + 1, element + 1 + (1 if offset > 0 else -1)] += abs(offset)
    return weights


def fit_series():
    nodes = np.cos((np.arange(64) + 0.5) * np.pi / 64)
    square = (nodes + 1.0) * 0.5 * np.pi**2
    root = np.sqrt(square)
    series = []
    for values in (np.sin(root) / root, np.cos(root)):
        fitted = np.polynomial.chebyshev.Chebyshev.fit(square, values, 8, domain=[0.0, np.pi**2])
        series.append(fitted.convert(kind=np.polynomial.Polynomial).coef)
    return series


SINE, COSINE = fit_series()


def horner(series, square):
    total = jnp.full_like(square, float(series[-1]))
    for coefficient in series[-2::-1]:
        total = total * square + float(coefficient)
    return total


def sine_cosine(angle):
    square = angle * angle
    return (angle * horner(SINE, square), horner(COSINE, square))


def parts_of(values, count):
    pieces = []
    for _ in range(count):
        piece = values.astype(jnp.bfloat16)
        pieces.append(piece)
        values = values - piece.astype(jnp.float32)
    return pieces


def dot(left, right):
    return jnp.dot(left, right, preferred_element_type=jnp.float32)


def fill_gradients(out_ref, start, deform_ref, slot_ref, rows):
    components, held = deform_ref.shape
    columns, coarse_depth = slot_ref.shape[1:]
    out_ref[start : start + rows, :] = jnp.zeros((rows, out_ref.shape[1]), jnp.float32)
    out_ref[start : start + components, 0:held] = deform_ref[...]
    out_ref[start + components : start + components + columns, 0:coarse_depth] = slot_ref[
        0
    ].astype(jnp.float32)


def pack_x(
    potential_ref, angle_ref, deform_ref, slot_ref, even_ref, odd_ref, even_bulk, odd_bulk, *, rows
):
    cells_x, cells_y = potential_ref.shape[:2]
    corner = deform_ref.shape[0] + slot_ref.shape[1]
    gx = lax.axis_index("gx")
    for out_ref, bulk_ref, goes_up in (
        (even_ref, even_bulk, gx % 2 == 0),
        (odd_ref, odd_bulk, gx % 2 == 1),
    ):
        fill_gradients(out_ref, 0, deform_ref, slot_ref, rows)
        sources = (potential_ref, angle_ref.at[0], angle_ref.at[1])
        for number, source in enumerate(sources):
            edge = jnp.where(goes_up, source[cells_x - 1], source[0])
            bulk_ref[number * cells_y : (number + 1) * cells_y] = edge
            if number == 0:
                out_ref[corner : corner + 1] = edge[0:1]
                out_ref[corner + 1 : corner + 2] = edge[cells_y - 1 :]


def pack_y(
    potential_ref, angle_ref, deform_ref, slot_ref, even_ref, odd_ref, *out_refs, rims, rows
):
    row_ref, plain_ref = out_refs[:2]
    cells_x, cells_y, depth = potential_ref.shape
    components = deform_ref.shape[0]
    columns, coarse_depth = slot_ref.shape[1:]
    corner = components + columns
    gx = lax.axis_index("gx")
    gy = lax.axis_index("gy")
    is_odd = gx % 2 == 1
    fill_gradients(row_ref, rows, deform_ref, slot_ref, rows)
    row_ref[rows + corner : rows + corner + 1] = potential_ref[0, 0:1]
    row_ref[rows + corner + 1 : rows + corner + 2] = potential_ref[0, cells_y - 1 :]
    own = row_ref[rows : 2 * rows]
    even, odd = even_ref[...], odd_ref[...]
    row_ref[0:rows] = jnp.where(gx == 0, own, jnp.where(is_odd, even, odd))
    row_ref[rows + corner : rows + corner + 1] = potential_ref[cells_x - 1, 0:1]
    row_ref[rows + corner + 1 : rows + corner + 2] = potential_ref[cells_x - 1, cells_y - 1 :]
    own = row_ref[rows : 2 * rows]
    at_last = gx == lax.axis_size("gx") - 1
    row_ref[2 * rows :] = jnp.where(at_last, own, jnp.where(is_odd, odd, even))
    plain_ref[3 * components :] = jnp.zeros(
        (plain_ref.shape[0] - 3 * components, depth), jnp.float32
    )
    for r in range(3):
        plain_ref[r * components : (r + 1) * components] = row_ref[r * rows : r * rows + components]
    first_rows = round_up(cells_x + 2, 8)
    for flips, out_ref in zip(rims, out_refs[2:]):
        goes_right = (gy ^ flips) > gy
        start = out_ref.shape[0] - plain_ref.shape[0]
        out_ref[start:] = plain_ref[...]
        out_ref[0:start] = jnp.zeros((start, depth), jnp.float32)
        for r in range(3):
            first = r * rows + components
            line = start + 3 * components + r
            out_ref[line : line + 1] = jnp.where(
                goes_right,
                row_ref[first + columns - 1 : first + columns],
                row_ref[first : first + 1],
            )
        for line, r in ((0, 0), (1 + cells_x, 2)):
            first = r * rows + corner
            out_ref[line : line + 1] = jnp.where(
                goes_right, row_ref[first + 1 : first + 2], row_ref[first : first + 1]
            )
        lines = []
        for x in range(cells_x):
            lines.append((1 + x, potential_ref.at[x]))
            lines.append((first_rows + x, angle_ref.at[0, x]))
            lines.append((first_rows + cells_x + x, angle_ref.at[1, x]))
        for line, source in lines:
            out_ref[line : line + 1] = jnp.where(
                goes_right, source[cells_y - 1 : cells_y], source[0:1]
            )


def tensors(entries, azimuth, elevation):
    sin_u, cos_u = sine_cosine(azimuth)
    sin_e, cos_e = sine_cosine(elevation)
    fiber = [cos_u * cos_e, sin_u * cos_e, sin_e]

    def element(row_index, col_index):
        return entries[3 * (row_index % 3) + col_index % 3]

    cofactor = [
        [
            element(row + 1, col + 1) * element(row + 2, col + 2)
            - element(row + 1, col + 2) * element(row + 2, col + 1)
            for col in range(3)
        ]
        for row in range(3)
    ]
    determinant = (
        element(0, 0) * cofactor[0][0]
        + element(0, 1) * cofactor[0][1]
        + element(0, 2) * cofactor[0][2]
    )
    scale = 1.0 / determinant
    adjugate = [[cofactor[col][row] for col in range(3)] for row in range(3)]
    pulled = [
        adjugate[row][0] * fiber[0] + adjugate[row][1] * fiber[1] + adjugate[row][2] * fiber[2]
        for row in range(3)
    ]
    cross = (scale * scale) * sigma_cross
    along = (scale * scale) * (sigma_fiber - sigma_cross)
    conduct = []
    for first, second in ((0, 0), (1, 1), (2, 2), (0, 1), (0, 2), (1, 2)):
        metric = (
            adjugate[first][0] * adjugate[second][0]
            + adjugate[first][1] * adjugate[second][1]
            + adjugate[first][2] * adjugate[second][2]
        )
        conduct.append(cross * metric + along * (pulled[first] * pulled[second]))
    return conduct, fiber


def stretch_of(entries, fiber):
    total = None
    for row in range(3):
        value = (
            entries[3 * row] * fiber[0]
            + entries[3 * row + 1] * fiber[1]
            + entries[3 * row + 2] * fiber[2]
        )
        total = value * value if total is None else total + value * value
    return jnp.sqrt(total)


def step(
    potential_ref,
    recovery_ref,
    angle_ref,
    even_ref,
    odd_ref,
    line_ref,
    side_ref,
    deep_ref,
    *refs,
    components,
    held,
    columns,
    coarse_depth,
    rows,
    devices,
):
    packets = refs[:devices]
    (
        potential_out,
        recovery_out,
        low_ref,
        high_ref,
        coarse_ref,
        fine_ref,
        conduct_ref,
        stretch_ref,
    ) = refs[devices:]
    cells_x, cells_y, depth = potential_ref.shape
    elements = cells_x // RATIO
    gx = lax.axis_index("gx")
    gy = lax.axis_index("gy")
    at_first_x = gx == 0
    at_last_x = gx == lax.axis_size("gx") - 1
    at_first_y = gy == 0
    at_last_y = gy == devices - 1
    rims = [flips for flips in range(1, devices) if is_rim(flips)]

    def beside(values, towards, own):
        chosen = own
        for flips, value in values.items():
            chosen = jnp.where((gy ^ flips) == towards, value, chosen)
        return chosen

    filler = jnp.zeros((rows - components, held), jnp.float32)
    skip = round_up(cells_x + 2, 8) + 2 * cells_x

    def table(r, flips):
        if flips == 0:
            return packets[0][r * rows : (r + 1) * rows]
        start = r * components + (skip if is_rim(flips) else 0)
        return jnp.concatenate([packets[flips][start : start + components], filler], axis=0)

    def facing(r, flips):
        start = skip + 3 * components + r
        return packets[flips][start : start + 1, 0 : 2 * coarse_depth]

    is_odd = gx % 2 == 1
    for number, source in enumerate((potential_ref, angle_ref.at[0], angle_ref.at[1])):
        part = slice(number * cells_y, (number + 1) * cells_y)
        even, odd = even_ref[part], odd_ref[part]
        low_ref[part] = jnp.where(at_first_x, source[0], jnp.where(is_odd, even, odd))
        high_ref[part] = jnp.where(at_last_x, source[cells_x - 1], jnp.where(is_odd, odd, even))

    first_rows = round_up(cells_x + 2, 8)
    rim_rows = []
    for side, towards in ((0, gy - 1), (cells_y - 1, gy + 1)):
        sources = [low_ref] + [potential_ref.at[x] for x in range(cells_x)] + [high_ref]
        own = [source[side : side + 1] for source in sources]
        own += [jnp.zeros_like(own[0])] * (first_rows - len(own))
        values = {flips: packets[flips][0:first_rows] for flips in rims}
        rim_rows.append(beside(values, towards, jnp.concatenate(own, axis=0)))
    rim_low, rim_high = rim_rows

    lanes = 2 * coarse_depth
    lane = lax.broadcasted_iota(jnp.int32, (1, lanes), 1)
    count = columns + 2
    gathered = [[None] * (count // 2) for _ in range(elements + 2)]
    for r in range(elements + 2):
        start = r * rows + components
        own = packets[0][start : start + columns, 0:lanes]
        values = {f: facing(r, f) for f in rims}
        before = beside(values, gy - 1, own[0:1])
        after = beside(values, gy + 1, own[columns - 1 : columns])
        line = [before] + [own[c : c + 1] for c in range(columns)] + [after]
        table_parts = parts_of(
            jnp.concatenate([table(r, f) for f in range(devices)], axis=0), 3
        )
        for pair in range(count // 2):
            slots = jnp.where(
                lane < coarse_depth,
                line[2 * pair],
                pltpu.roll(line[2 * pair + 1], coarse_depth, 1),
            ).astype(jnp.int32)
            place = slots % held
            flips_of = ((slots // held) % devices) ^ gy
            match = lax.broadcasted_iota(jnp.int32, (held, lanes), 0) == place
            chosen = jnp.where(match, 1.0, 0.0).astype(jnp.bfloat16)
            values = dot(table_parts[0], chosen)
            for part in table_parts[1:]:
                values = values + dot(part, chosen)
            picked = values[0:rows]
            for flips in range(1, devices):
                picked = jnp.where(
                    flips_of == flips, values[flips * rows : (flips + 1) * rows], picked
                )
            gathered[r][pair] = picked

    tall = (elements + 2) * rows
    for pair in range(count // 2):
        stacked = jnp.concatenate([gathered[r][pair] for r in range(elements + 2)], axis=0)
        values = None
        for part in parts_of(stacked, 3):
            term = dot(part, deep_ref[...])
            values = term if values is None else values + term
        coarse_ref[2 * pair * tall : (2 * pair + 1) * tall] = values[:, 0:depth]
        coarse_ref[(2 * pair + 1) * tall : (2 * pair + 2) * tall] = values[:, depth : 2 * depth]
    block_rows = cells_y * components
    along_x = interpolation(elements)
    blended = []
    for x in range(cells_x + 2):
        columns_x = []
        for c in range(count):
            total = None
            for r in range(elements + 2):
                weight = float(along_x[x, r])
                if weight:
                    start = c * tall + r * rows
                    term = weight * coarse_ref[start : start + rows]
                    total = term if total is None else total + term
            columns_x.append(total)
        pieces = parts_of(jnp.concatenate(columns_x, axis=0), 2)
        blended.append(pieces)
        place = x - 1 if 0 < x <= cells_x else (cells_x if x == 0 else cells_x + 1)
        fine_ref[place * block_rows : (place + 1) * block_rows] = dot(
            line_ref[...], pieces[0]
        ) + dot(line_ref[...], pieces[1])
    side_base = (cells_x + 2) * block_rows
    total = None
    for number in range(2):
        stacked = jnp.concatenate([blended[x + 1][number] for x in range(cells_x)], axis=0)
        term = dot(side_ref[...], stacked)
        total = term if total is None else total + term
    fine_ref[side_base:] = total

    total_rows = fine_ref.shape[0] // components
    inner_rows = cells_x * cells_y
    chunk = 8
    for start in range(0, total_rows, chunk):
        if start < inner_rows + 2 * cells_y:
            base, stride = start // cells_y * block_rows + start % cells_y, cells_y
        else:
            base, stride = side_base, total_rows - inner_rows - 2 * cells_y
        entries = [
            fine_ref[base + k * stride : base + k * stride + chunk] for k in range(components)
        ]
        if start < inner_rows:
            x, y = start // cells_y, start % cells_y
            azimuth = angle_ref[0, x, y : y + chunk]
            elevation = angle_ref[1, x, y : y + chunk]
        elif start < inner_rows + 2 * cells_y:
            edge_ref = low_ref if start < inner_rows + cells_y else high_ref
            y = (start - inner_rows) % cells_y
            azimuth = edge_ref[cells_y + y : cells_y + y + chunk]
            elevation = edge_ref[2 * cells_y + y : 2 * cells_y + y + chunk]
        else:
            pieces = [[], []]
            for number in range(2):
                first = first_rows + number * cells_x
                for towards in (gy - 1, gy + 1):
                    values = {f: packets[f][first : first + cells_x] for f in rims}
                    pieces[number].append(beside(values, towards, values[rims[0]]))
            azimuth = jnp.concatenate(pieces[0], axis=0)
            elevation = jnp.concatenate(pieces[1], axis=0)
        conduct, fiber = tensors(entries, azimuth, elevation)
        for number in range(6):
            conduct_ref[number, start : start + chunk] = conduct[number]
        if start < inner_rows:
            stretch_ref[start : start + chunk] = stretch_of(entries, fiber)

    row_index = lax.broadcasted_iota(jnp.int32, (cells_y, depth), 0)
    lane_index = lax.broadcasted_iota(jnp.int32, (cells_y, depth), 1)
    def deeper(values, first):
        return jnp.where(first, values, pltpu.roll(values, 1, 1))

    def grad_z(values):
        index = lax.broadcasted_iota(jnp.int32, values.shape, 1)
        after = jnp.where(index == depth - 1, values, pltpu.roll(values, depth - 1, 1))
        before = jnp.where(index == 0, values, pltpu.roll(values, 1, 1))
        return (after - before) * 0.5

    def lower_y(values, rim):
        return jnp.where(row_index == 0, rim, pltpu.roll(values, 1, 0))

    def upper_y(values, rim):
        return jnp.where(row_index == cells_y - 1, rim, pltpu.roll(values, cells_y - 1, 0))

    def voltage_at(x):
        if x < 0:
            return low_ref[0:cells_y]
        if x >= cells_x:
            return high_ref[0:cells_y]
        return potential_ref[x]

    def conduct_at(number, x):
        if x < 0:
            return conduct_ref[number, inner_rows : inner_rows + cells_y]
        if x >= cells_x:
            return conduct_ref[number, inner_rows + cells_y : inner_rows + 2 * cells_y]
        return conduct_ref[number, x * cells_y : (x + 1) * cells_y]

    voltages = [voltage_at(x) for x in range(-1, cells_x + 1)]
    grads_y = [
        (
            upper_y(voltages[x], rim_high[x : x + 1])
            - lower_y(voltages[x], rim_low[x : x + 1])
        )
        * 0.5
        for x in range(cells_x + 2)
    ]
    grads_z = [grad_z(values) for values in voltages]
    rim_z = [grad_z(rim_low), grad_z(rim_high)]

    def flux(tensor_a, tensor_b, grads_a, grads_b, straight, voltage_a, voltage_b):
        total = None
        for place in range(3):
            mean = (tensor_a[place] + tensor_b[place]) * 0.5
            if place == straight:
                term = mean * (voltage_b - voltage_a)
            else:
                term = mean * ((grads_a[place] + grads_b[place]) * 0.5)
            total = term if total is None else total + term
        return total

    flux_x = []
    for face in range(cells_x + 1):
        value = flux(
            [conduct_at(n, face - 1) for n in (0, 3, 4)],
            [conduct_at(n, face) for n in (0, 3, 4)],
            [None, grads_y[face], grads_z[face]],
            [None, grads_y[face + 1], grads_z[face + 1]],
            0,
            voltages[face],
            voltages[face + 1],
        )
        if face == 0:
            value = jnp.where(at_first_x, 0.0, value)
        if face == cells_x:
            value = jnp.where(at_last_x, 0.0, value)
        flux_x.append(value)

    rim_start = inner_rows + 2 * cells_y
    for x in range(cells_x):
        voltage = voltages[x + 1]
        grad_x = (voltages[x + 2] - voltages[x]) * 0.5
        grad_y = grads_y[x + 1]
        grad_zz = grads_z[x + 1]
        tensor = [conduct_at(n, x) for n in (3, 1, 5)]
        low_tensor = [conduct_ref[n, rim_start + x : rim_start + x + 1] for n in (3, 1, 5)]
        high_tensor = [
            conduct_ref[n, rim_start + cells_x + x : rim_start + cells_x + x + 1]
            for n in (3, 1, 5)
        ]
        low_grads = [
            (rim_low[x + 2 : x + 3] - rim_low[x : x + 1]) * 0.5,
            None,
            rim_z[0][x + 1 : x + 2],
        ]
        high_grads = [
            (rim_high[x + 2 : x + 3] - rim_high[x : x + 1]) * 0.5,
            None,
            rim_z[1][x + 1 : x + 2],
        ]
        lower = flux(
            [lower_y(tensor[n], low_tensor[n]) for n in range(3)],
            tensor,
            [lower_y(grad_x, low_grads[0]), None, lower_y(grad_zz, low_grads[2])],
            [grad_x, None, grad_zz],
            1,
            lower_y(voltage, rim_low[x + 1 : x + 2]),
            voltage,
        )
        lower = jnp.where((row_index == 0) & at_first_y, 0.0, lower)
        top = flux(
            [value[cells_y - 1 : cells_y] for value in tensor],
            high_tensor,
            [grad_x[cells_y - 1 : cells_y], None, grad_zz[cells_y - 1 : cells_y]],
            high_grads,
            1,
            voltage[cells_y - 1 : cells_y],
            rim_high[x + 1 : x + 2],
        )
        top = jnp.where(at_last_y, 0.0, top)
        divergent = flux_x[x + 1] - flux_x[x] + (upper_y(lower, top) - lower)
        first = lane_index == 0
        tensor = [conduct_at(n, x) for n in (4, 5, 2)]
        before = flux(
            [deeper(value, first) for value in tensor],
            tensor,
            [deeper(grad_x, first), deeper(grad_y, first), None],
            [grad_x, grad_y, None],
            2,
            deeper(voltage, first),
            voltage,
        )
        before = jnp.where(first, 0.0, before)
        divergent = divergent + (pltpu.roll(before, depth - 1, 1) - before)
        recovery = recovery_ref[x]
        stretch = stretch_ref[x * cells_y : (x + 1) * cells_y]
        current = (
            excite_gain * voltage * (voltage - excite_level) * (voltage - 1.0)
            + voltage * recovery
        )
        current = current + stretch_gain * jnp.maximum(stretch - 1.0, 0.0) * (
            voltage - stretch_reversal
        )
        potential_out[x] = voltage + time_step * (divergent - current)
        recovery_out[x] = recovery + time_step * recover_rate * (
            -recovery - excite_gain * voltage * (voltage - excite_level - 1.0)
        )


def weights_of(cells_x, cells_y, columns, coarse_depth, depth, rows, components):
    deep = np.zeros((coarse_depth, depth))
    along_z = interpolation(coarse_depth)[1:-1]
    deep += along_z[:, 1:-1].T
    deep[0] += along_z[:, 0]
    deep[-1] += along_z[:, -1]
    pair = np.zeros((2 * coarse_depth, 2 * depth))
    pair[:coarse_depth, :depth] = deep
    pair[coarse_depth:, depth:] = deep
    along_y = interpolation(columns)
    line = np.zeros((components, cells_y, columns + 2, rows))
    side = np.zeros((components, 2, cells_x, cells_x, columns + 2, rows))
    for k in range(components):
        line[k, :, :, k] = along_y[1:-1]
        for x in range(cells_x):
            side[k, 0, x, x, :, k] = along_y[0]
            side[k, 1, x, x, :, k] = along_y[-1]
    line = line.reshape(components * cells_y, -1)
    side = side.reshape(components * 2 * cells_x, -1)
    return [jnp.asarray(values, jnp.bfloat16) for values in (line, side, pair)]


def is_rim(flips):
    return flips > 0 and flips & (flips + 1) == 0


def local(potential, recovery, fiber_angles, deform, elem_slot):
    cells_x, cells_y, depth = potential.shape
    elements, columns, coarse_depth = elem_slot.shape
    components, held = deform.shape
    rows = round_up(components + columns + 2, 8)
    weights = weights_of(cells_x, cells_y, columns, coarse_depth, depth, rows, components)
    across, down = lax.axis_size("gx"), lax.axis_size("gy")
    assert elements == 1 and columns % 2 == 0 and held == depth
    assert down & (down - 1) == 0 and down > 1 and 2 * cells_x == 8

    def packet(count):
        return OUT((count, depth))

    arrays = (potential, fiber_angles, deform, elem_slot)
    swaps = [[(x, x ^ 1) for x in range(across) if x ^ 1 < across]]
    upward = [(x, x + 1) for x in range(1, across - 1, 2)]
    swaps.append(upward + [(high, low) for low, high in upward])
    even, odd, even_bulk, odd_bulk = pl.pallas_call(
        functools.partial(pack_x, rows=rows),
        out_shape=[packet(rows)] * 2 + [packet(3 * cells_y)] * 2,
        name="pack_x",
    )(*arrays)
    odd = lax.ppermute(odd, "gx", swaps[1])
    even = lax.ppermute(even, "gx", swaps[0])
    odd_bulk = lax.ppermute(odd_bulk, "gx", swaps[1])
    even_bulk = lax.ppermute(even_bulk, "gx", swaps[0])
    rims = [flips for flips in range(1, down) if is_rim(flips)]
    side_rows = round_up(cells_x + 2, 8) + 2 * cells_x
    plain_rows = round_up(3 * components + 3, 8)
    row, plain, *sent = pl.pallas_call(
        functools.partial(pack_y, rims=rims, rows=rows),
        out_shape=[packet(3 * rows), packet(plain_rows)]
        + [packet(side_rows + plain_rows)] * len(rims),
        name="pack_y",
    )(*[IN(value) for value in arrays], IN(even), IN(odd))
    sent = dict(zip(rims, sent))
    packets = [IN(row)]
    for flips in range(1, down):
        pairs = [(y, y ^ flips) for y in range(down)]
        packets.append(IN(lax.ppermute(sent.get(flips, plain), "gy", pairs)))
    block = jax.ShapeDtypeStruct((cells_x, cells_y, depth), jnp.float32)
    line_count = (cells_x + 2) * cells_y + 2 * cells_x
    return pl.pallas_call(
        functools.partial(
            step,
            components=components,
            held=held,
            columns=columns,
            coarse_depth=coarse_depth,
            rows=rows,
            devices=down,
        ),
        out_shape=(block, block),
        scratch_shapes=[
            pltpu.VMEM((3 * cells_y, depth), jnp.float32),
            pltpu.VMEM((3 * cells_y, depth), jnp.float32),
            pltpu.VMEM(((columns + 2) * (elements + 2) * rows, depth), jnp.float32),
            pltpu.VMEM((components * line_count, depth), jnp.float32),
            pltpu.VMEM((6, line_count, depth), jnp.float32),
            pltpu.VMEM((cells_x * cells_y, depth), jnp.float32),
        ],
        name="step",
    )(
        IN(potential),
        IN(recovery),
        IN(fiber_angles),
        IN(even_bulk),
        IN(odd_bulk),
        weights[0],
        *[IN(value) for value in weights[1:]],
        *packets,
    )


def solution(mesh):
    placed = (
        P("gx", "gy", None),
        P("gx", "gy", None),
        P(None, "gx", "gy", None),
        P(None, ("gx", "gy")),
        P("gx", "gy", None),
    )
    return jax.shard_map(
        local,
        mesh=mesh,
        in_specs=placed,
        out_specs=(P("gx", "gy", None), P("gx", "gy", None)),
        check_vma=False,
    )
```

```python
import functools

import jax
import jax.numpy as jnp
import numpy as np
from jax import lax
from jax.experimental import pallas as pl
from jax.experimental.pallas import tpu as pltpu
from jax.sharding import PartitionSpec as P

RATIO = 4

sigma_fiber = 1.0
sigma_cross = 0.3
time_step = 0.1
excite_gain = 8.0
excite_level = 0.15
stretch_gain = 10.0
stretch_reversal = 0.6
recover_rate = 0.5


def IN(values):
    return pltpu.with_memory_space_constraint(values, pltpu.VMEM)


def OUT(shape):
    return pltpu.VMEM(shape, jnp.float32)


def round_up(value, multiple):
    return -(-value // multiple) * multiple


def interpolation(count):
    weights = np.zeros((RATIO * count + 2, count + 2))
    for cell in range(-1, RATIO * count + 1):
        element, position = cell // RATIO, cell % RATIO
        offset = (position + 0.5) / RATIO - 0.5
        weights[cell + 1, element + 1] += 1.0 - abs(offset)
        weights[cell + 1, element + 1 + (1 if offset > 0 else -1)] += abs(offset)
    return weights


def fit_series():
    nodes = np.cos((np.arange(64) + 0.5) * np.pi / 64)
    square = (nodes + 1.0) * 0.5 * np.pi**2
    root = np.sqrt(square)
    series = []
    for values in (np.sin(root) / root, np.cos(root)):
        fitted = np.polynomial.chebyshev.Chebyshev.fit(square, values, 8, domain=[0.0, np.pi**2])
        series.append(fitted.convert(kind=np.polynomial.Polynomial).coef)
    return series


SINE, COSINE = fit_series()


def horner(series, square):
    total = jnp.full_like(square, float(series[-1]))
    for coefficient in series[-2::-1]:
        total = total * square + float(coefficient)
    return total


def sine_cosine(angle):
    square = angle * angle
    return (angle * horner(SINE, square), horner(COSINE, square))


def parts_of(values, count):
    pieces = []
    for _ in range(count):
        piece = values.astype(jnp.bfloat16)
        pieces.append(piece)
        values = values - piece.astype(jnp.float32)
    return pieces


def dot(left, right):
    return jnp.dot(left, right, preferred_element_type=jnp.float32)


def fill_gradients(out_ref, start, deform_ref, slot_ref, rows):
    components, held = deform_ref.shape
    columns, coarse_depth = slot_ref.shape[1:]
    out_ref[start : start + rows, :] = jnp.zeros((rows, out_ref.shape[1]), jnp.float32)
    out_ref[start : start + components, 0:held] = deform_ref[...]
    out_ref[start + components : start + components + columns, 0:coarse_depth] = slot_ref[
        0
    ].astype(jnp.float32)


def pack_x(potential_ref, deform_ref, slot_ref, even_ref, odd_ref, *, rows):
    cells_x, cells_y = potential_ref.shape[:2]
    corner = deform_ref.shape[0] + slot_ref.shape[1]
    gx = lax.axis_index("gx")
    for out_ref, goes_up in ((even_ref, gx % 2 == 0), (odd_ref, gx % 2 == 1)):
        fill_gradients(out_ref, 0, deform_ref, slot_ref, rows)
        for line, y in ((corner, 0), (corner + 1, cells_y - 1)):
            out_ref[line : line + 1] = jnp.where(
                goes_up, potential_ref[cells_x - 1, y : y + 1], potential_ref[0, y : y + 1]
            )


def pack_y(
    potential_ref, angle_ref, deform_ref, slot_ref, even_ref, odd_ref, *out_refs, rims, rows
):
    row_ref, plain_ref, even_bulk, odd_bulk = out_refs[:4]
    cells_x, cells_y, depth = potential_ref.shape
    components = deform_ref.shape[0]
    columns, coarse_depth = slot_ref.shape[1:]
    corner = components + columns
    gx = lax.axis_index("gx")
    gy = lax.axis_index("gy")
    is_odd = gx % 2 == 1
    for bulk_ref, goes_up in ((even_bulk, gx % 2 == 0), (odd_bulk, gx % 2 == 1)):
        for number, source in enumerate((potential_ref, angle_ref.at[0], angle_ref.at[1])):
            bulk_ref[number * cells_y : (number + 1) * cells_y] = jnp.where(
                goes_up, source[cells_x - 1], source[0]
            )
    fill_gradients(row_ref, rows, deform_ref, slot_ref, rows)
    row_ref[rows + corner : rows + corner + 1] = potential_ref[0, 0:1]
    row_ref[rows + corner + 1 : rows + corner + 2] = potential_ref[0, cells_y - 1 :]
    own = row_ref[rows : 2 * rows]
    even, odd = even_ref[...], odd_ref[...]
    row_ref[0:rows] = jnp.where(gx == 0, own, jnp.where(is_odd, even, odd))
    row_ref[rows + corner : rows + corner + 1] = potential_ref[cells_x - 1, 0:1]
    row_ref[rows + corner + 1 : rows + corner + 2] = potential_ref[cells_x - 1, cells_y - 1 :]
    own = row_ref[rows : 2 * rows]
    at_last = gx == lax.axis_size("gx") - 1
    row_ref[2 * rows :] = jnp.where(at_last, own, jnp.where(is_odd, odd, even))
    plain_ref[3 * components :] = jnp.zeros(
        (plain_ref.shape[0] - 3 * components, depth), jnp.float32
    )
    for r in range(3):
        plain_ref[r * components : (r + 1) * components] = row_ref[r * rows : r * rows + components]
    first_rows = round_up(cells_x + 2, 8)
    for flips, out_ref in zip(rims, out_refs[4:]):
        goes_right = (gy ^ flips) > gy
        start = out_ref.shape[0] - plain_ref.shape[0]
        out_ref[start:] = plain_ref[...]
        out_ref[0:start] = jnp.zeros((start, depth), jnp.float32)
        for r in range(3):
            first = r * rows + components
            line = start + 3 * components + r
            out_ref[line : line + 1] = jnp.where(
                goes_right,
                row_ref[first + columns - 1 : first + columns],
                row_ref[first : first + 1],
            )
        for line, r in ((0, 0), (1 + cells_x, 2)):
            first = r * rows + corner
            out_ref[line : line + 1] = jnp.where(
                goes_right, row_ref[first + 1 : first + 2], row_ref[first : first + 1]
            )
        lines = []
        for x in range(cells_x):
            lines.append((1 + x, potential_ref.at[x]))
            lines.append((first_rows + x, angle_ref.at[0, x]))
            lines.append((first_rows + cells_x + x, angle_ref.at[1, x]))
        for line, source in lines:
            out_ref[line : line + 1] = jnp.where(
                goes_right, source[cells_y - 1 : cells_y], source[0:1]
            )


def tensors(entries, azimuth, elevation):
    sin_u, cos_u = sine_cosine(azimuth)
    sin_e, cos_e = sine_cosine(elevation)
    fiber = [cos_u * cos_e, sin_u * cos_e, sin_e]

    def element(row_index, col_index):
        return entries[3 * (row_index % 3) + col_index % 3]

    cofactor = [
        [
            element(row + 1, col + 1) * element(row + 2, col + 2)
            - element(row + 1, col + 2) * element(row + 2, col + 1)
            for col in range(3)
        ]
        for row in range(3)
    ]
    determinant = (
        element(0, 0) * cofactor[0][0]
        + element(0, 1) * cofactor[0][1]
        + element(0, 2) * cofactor[0][2]
    )
    scale = 1.0 / determinant
    adjugate = [[cofactor[col][row] for col in range(3)] for row in range(3)]
    pulled = [
        adjugate[row][0] * fiber[0] + adjugate[row][1] * fiber[1] + adjugate[row][2] * fiber[2]
        for row in range(3)
    ]
    cross = (scale * scale) * sigma_cross
    along = (scale * scale) * (sigma_fiber - sigma_cross)
    conduct = []
    for first, second in ((0, 0), (1, 1), (2, 2), (0, 1), (0, 2), (1, 2)):
        metric = (
            adjugate[first][0] * adjugate[second][0]
            + adjugate[first][1] * adjugate[second][1]
            + adjugate[first][2] * adjugate[second][2]
        )
        conduct.append(cross * metric + along * (pulled[first] * pulled[second]))
    return conduct, fiber


def stretch_of(entries, fiber):
    total = None
    for row in range(3):
        value = (
            entries[3 * row] * fiber[0]
            + entries[3 * row + 1] * fiber[1]
            + entries[3 * row + 2] * fiber[2]
        )
        total = value * value if total is None else total + value * value
    return jnp.sqrt(total)


def step(
    potential_ref,
    recovery_ref,
    angle_ref,
    even_ref,
    odd_ref,
    line_ref,
    side_ref,
    deep_ref,
    *refs,
    components,
    held,
    columns,
    coarse_depth,
    rows,
    devices,
):
    packets = refs[:devices]
    (
        potential_out,
        recovery_out,
        low_ref,
        high_ref,
        coarse_ref,
        fine_ref,
        conduct_ref,
        stretch_ref,
    ) = refs[devices:]
    cells_x, cells_y, depth = potential_ref.shape
    elements = cells_x // RATIO
    gx = lax.axis_index("gx")
    gy = lax.axis_index("gy")
    at_first_x = gx == 0
    at_last_x = gx == lax.axis_size("gx") - 1
    at_first_y = gy == 0
    at_last_y = gy == devices - 1
    rims = [flips for flips in range(1, devices) if is_rim(flips)]

    def beside(values, towards, own):
        chosen = own
        for flips, value in values.items():
            chosen = jnp.where((gy ^ flips) == towards, value, chosen)
        return chosen

    filler = jnp.zeros((rows - components, held), jnp.float32)
    skip = round_up(cells_x + 2, 8) + 2 * cells_x

    def table(r, flips):
        if flips == 0:
            return packets[0][r * rows : (r + 1) * rows]
        start = r * components + (skip if is_rim(flips) else 0)
        return jnp.concatenate([packets[flips][start : start + components], filler], axis=0)

    def facing(r, flips):
        start = skip + 3 * components + r
        return packets[flips][start : start + 1, 0 : 2 * coarse_depth]

    is_odd = gx % 2 == 1
    for number, source in enumerate((potential_ref, angle_ref.at[0], angle_ref.at[1])):
        part = slice(number * cells_y, (number + 1) * cells_y)
        even, odd = even_ref[part], odd_ref[part]
        low_ref[part] = jnp.where(at_first_x, source[0], jnp.where(is_odd, even, odd))
        high_ref[part] = jnp.where(at_last_x, source[cells_x - 1], jnp.where(is_odd, odd, even))

    first_rows = round_up(cells_x + 2, 8)
    rim_rows = []
    for side, towards in ((0, gy - 1), (cells_y - 1, gy + 1)):
        sources = [low_ref] + [potential_ref.at[x] for x in range(cells_x)] + [high_ref]
        own = [source[side : side + 1] for source in sources]
        own += [jnp.zeros_like(own[0])] * (first_rows - len(own))
        values = {flips: packets[flips][0:first_rows] for flips in rims}
        rim_rows.append(beside(values, towards, jnp.concatenate(own, axis=0)))
    rim_low, rim_high = rim_rows

    lanes = 2 * coarse_depth
    lane = lax.broadcasted_iota(jnp.int32, (1, lanes), 1)
    count = columns + 2
    gathered = [[None] * (count // 2) for _ in range(elements + 2)]
    for r in range(elements + 2):
        start = r * rows + components
        own = packets[0][start : start + columns, 0:lanes]
        values = {f: facing(r, f) for f in rims}
        before = beside(values, gy - 1, own[0:1])
        after = beside(values, gy + 1, own[columns - 1 : columns])
        line = [before] + [own[c : c + 1] for c in range(columns)] + [after]
        table_parts = parts_of(
            jnp.concatenate([table(r, f) for f in range(devices)], axis=0), 3
        )
        for pair in range(count // 2):
            slots = jnp.where(
                lane < coarse_depth,
                line[2 * pair],
                pltpu.roll(line[2 * pair + 1], coarse_depth, 1),
            ).astype(jnp.int32)
            place = slots % held
            flips_of = ((slots // held) % devices) ^ gy
            match = lax.broadcasted_iota(jnp.int32, (held, lanes), 0) == place
            chosen = jnp.where(match, 1.0, 0.0).astype(jnp.bfloat16)
            values = dot(table_parts[0], chosen)
            for part in table_parts[1:]:
                values = values + dot(part, chosen)
            picked = values[0:rows]
            for flips in range(1, devices):
                picked = jnp.where(
                    flips_of == flips, values[flips * rows : (flips + 1) * rows], picked
                )
            gathered[r][pair] = picked

    tall = (elements + 2) * rows
    for pair in range(count // 2):
        stacked = jnp.concatenate([gathered[r][pair] for r in range(elements + 2)], axis=0)
        values = None
        for part in parts_of(stacked, 3):
            term = dot(part, deep_ref[...])
            values = term if values is None else values + term
        coarse_ref[2 * pair * tall : (2 * pair + 1) * tall] = values[:, 0:depth]
        coarse_ref[(2 * pair + 1) * tall : (2 * pair + 2) * tall] = values[:, depth : 2 * depth]
    block_rows = cells_y * components
    along_x = interpolation(elements)
    blended = []
    for x in range(cells_x + 2):
        columns_x = []
        for c in range(count):
            total = None
            for r in range(elements + 2):
                weight = float(along_x[x, r])
                if weight:
                    start = c * tall + r * rows
                    term = weight * coarse_ref[start : start + rows]
                    total = term if total is None else total + term
            columns_x.append(total)
        pieces = parts_of(jnp.concatenate(columns_x, axis=0), 2)
        blended.append(pieces)
        place = x - 1 if 0 < x <= cells_x else (cells_x if x == 0 else cells_x + 1)
        fine_ref[place * block_rows : (place + 1) * block_rows] = dot(
            line_ref[...], pieces[0]
        ) + dot(line_ref[...], pieces[1])
    side_base = (cells_x + 2) * block_rows
    total = None
    for number in range(2):
        stacked = jnp.concatenate([blended[x + 1][number] for x in range(cells_x)], axis=0)
        term = dot(side_ref[...], stacked)
        total = term if total is None else total + term
    fine_ref[side_base:] = total

    total_rows = fine_ref.shape[0] // components
    inner_rows = cells_x * cells_y
    chunk = 8
    for start in range(0, total_rows, chunk):
        if start < inner_rows + 2 * cells_y:
            base, stride = start // cells_y * block_rows + start % cells_y, cells_y
        else:
            base, stride = side_base, total_rows - inner_rows - 2 * cells_y
        entries = [
            fine_ref[base + k * stride : base + k * stride + chunk] for k in range(components)
        ]
        if start < inner_rows:
            x, y = start // cells_y, start % cells_y
            azimuth = angle_ref[0, x, y : y + chunk]
            elevation = angle_ref[1, x, y : y + chunk]
        elif start < inner_rows + 2 * cells_y:
            edge_ref = low_ref if start < inner_rows + cells_y else high_ref
            y = (start - inner_rows) % cells_y
            azimuth = edge_ref[cells_y + y : cells_y + y + chunk]
            elevation = edge_ref[2 * cells_y + y : 2 * cells_y + y + chunk]
        else:
            pieces = [[], []]
            for number in range(2):
                first = first_rows + number * cells_x
                for towards in (gy - 1, gy + 1):
                    values = {f: packets[f][first : first + cells_x] for f in rims}
                    pieces[number].append(beside(values, towards, values[rims[0]]))
            azimuth = jnp.concatenate(pieces[0], axis=0)
            elevation = jnp.concatenate(pieces[1], axis=0)
        conduct, fiber = tensors(entries, azimuth, elevation)
        for number in range(6):
            conduct_ref[number, start : start + chunk] = conduct[number]
        if start < inner_rows:
            stretch_ref[start : start + chunk] = stretch_of(entries, fiber)

    row_index = lax.broadcasted_iota(jnp.int32, (cells_y, depth), 0)
    lane_index = lax.broadcasted_iota(jnp.int32, (cells_y, depth), 1)
    def deeper(values, first):
        return jnp.where(first, values, pltpu.roll(values, 1, 1))

    def grad_z(values):
        index = lax.broadcasted_iota(jnp.int32, values.shape, 1)
        after = jnp.where(index == depth - 1, values, pltpu.roll(values, depth - 1, 1))
        before = jnp.where(index == 0, values, pltpu.roll(values, 1, 1))
        return (after - before) * 0.5

    def lower_y(values, rim):
        return jnp.where(row_index == 0, rim, pltpu.roll(values, 1, 0))

    def upper_y(values, rim):
        return jnp.where(row_index == cells_y - 1, rim, pltpu.roll(values, cells_y - 1, 0))

    def voltage_at(x):
        if x < 0:
            return low_ref[0:cells_y]
        if x >= cells_x:
            return high_ref[0:cells_y]
        return potential_ref[x]

    def conduct_at(number, x):
        if x < 0:
            return conduct_ref[number, inner_rows : inner_rows + cells_y]
        if x >= cells_x:
            return conduct_ref[number, inner_rows + cells_y : inner_rows + 2 * cells_y]
        return conduct_ref[number, x * cells_y : (x + 1) * cells_y]

    voltages = [voltage_at(x) for x in range(-1, cells_x + 1)]
    grads_y = [
        (
            upper_y(voltages[x], rim_high[x : x + 1])
            - lower_y(voltages[x], rim_low[x : x + 1])
        )
        * 0.5
        for x in range(cells_x + 2)
    ]
    grads_z = [grad_z(values) for values in voltages]
    rim_z = [grad_z(rim_low), grad_z(rim_high)]

    def flux(tensor_a, tensor_b, grads_a, grads_b, straight, voltage_a, voltage_b):
        total = None
        for place in range(3):
            mean = (tensor_a[place] + tensor_b[place]) * 0.5
            if place == straight:
                term = mean * (voltage_b - voltage_a)
            else:
                term = mean * ((grads_a[place] + grads_b[place]) * 0.5)
            total = term if total is None else total + term
        return total

    flux_x = []
    for face in range(cells_x + 1):
        value = flux(
            [conduct_at(n, face - 1) for n in (0, 3, 4)],
            [conduct_at(n, face) for n in (0, 3, 4)],
            [None, grads_y[face], grads_z[face]],
            [None, grads_y[face + 1], grads_z[face + 1]],
            0,
            voltages[face],
            voltages[face + 1],
        )
        if face == 0:
            value = jnp.where(at_first_x, 0.0, value)
        if face == cells_x:
            value = jnp.where(at_last_x, 0.0, value)
        flux_x.append(value)

    rim_start = inner_rows + 2 * cells_y
    for x in range(cells_x):
        voltage = voltages[x + 1]
        grad_x = (voltages[x + 2] - voltages[x]) * 0.5
        grad_y = grads_y[x + 1]
        grad_zz = grads_z[x + 1]
        tensor = [conduct_at(n, x) for n in (3, 1, 5)]
        low_tensor = [conduct_ref[n, rim_start + x : rim_start + x + 1] for n in (3, 1, 5)]
        high_tensor = [
            conduct_ref[n, rim_start + cells_x + x : rim_start + cells_x + x + 1]
            for n in (3, 1, 5)
        ]
        low_grads = [
            (rim_low[x + 2 : x + 3] - rim_low[x : x + 1]) * 0.5,
            None,
            rim_z[0][x + 1 : x + 2],
        ]
        high_grads = [
            (rim_high[x + 2 : x + 3] - rim_high[x : x + 1]) * 0.5,
            None,
            rim_z[1][x + 1 : x + 2],
        ]
        lower = flux(
            [lower_y(tensor[n], low_tensor[n]) for n in range(3)],
            tensor,
            [lower_y(grad_x, low_grads[0]), None, lower_y(grad_zz, low_grads[2])],
            [grad_x, None, grad_zz],
            1,
            lower_y(voltage, rim_low[x + 1 : x + 2]),
            voltage,
        )
        lower = jnp.where((row_index == 0) & at_first_y, 0.0, lower)
        top = flux(
            [value[cells_y - 1 : cells_y] for value in tensor],
            high_tensor,
            [grad_x[cells_y - 1 : cells_y], None, grad_zz[cells_y - 1 : cells_y]],
            high_grads,
            1,
            voltage[cells_y - 1 : cells_y],
            rim_high[x + 1 : x + 2],
        )
        top = jnp.where(at_last_y, 0.0, top)
        divergent = flux_x[x + 1] - flux_x[x] + (upper_y(lower, top) - lower)
        first = lane_index == 0
        tensor = [conduct_at(n, x) for n in (4, 5, 2)]
        before = flux(
            [deeper(value, first) for value in tensor],
            tensor,
            [deeper(grad_x, first), deeper(grad_y, first), None],
            [grad_x, grad_y, None],
            2,
            deeper(voltage, first),
            voltage,
        )
        before = jnp.where(first, 0.0, before)
        divergent = divergent + (pltpu.roll(before, depth - 1, 1) - before)
        recovery = recovery_ref[x]
        stretch = stretch_ref[x * cells_y : (x + 1) * cells_y]
        current = (
            excite_gain * voltage * (voltage - excite_level) * (voltage - 1.0)
            + voltage * recovery
        )
        current = current + stretch_gain * jnp.maximum(stretch - 1.0, 0.0) * (
            voltage - stretch_reversal
        )
        potential_out[x] = voltage + time_step * (divergent - current)
        recovery_out[x] = recovery + time_step * recover_rate * (
            -recovery - excite_gain * voltage * (voltage - excite_level - 1.0)
        )


def weights_of(cells_x, cells_y, columns, coarse_depth, depth, rows, components):
    deep = np.zeros((coarse_depth, depth))
    along_z = interpolation(coarse_depth)[1:-1]
    deep += along_z[:, 1:-1].T
    deep[0] += along_z[:, 0]
    deep[-1] += along_z[:, -1]
    pair = np.zeros((2 * coarse_depth, 2 * depth))
    pair[:coarse_depth, :depth] = deep
    pair[coarse_depth:, depth:] = deep
    along_y = interpolation(columns)
    line = np.zeros((components, cells_y, columns + 2, rows))
    side = np.zeros((components, 2, cells_x, cells_x, columns + 2, rows))
    for k in range(components):
        line[k, :, :, k] = along_y[1:-1]
        for x in range(cells_x):
            side[k, 0, x, x, :, k] = along_y[0]
            side[k, 1, x, x, :, k] = along_y[-1]
    line = line.reshape(components * cells_y, -1)
    side = side.reshape(components * 2 * cells_x, -1)
    return [jnp.asarray(values, jnp.bfloat16) for values in (line, side, pair)]


def is_rim(flips):
    return flips > 0 and flips & (flips + 1) == 0


def local(potential, recovery, fiber_angles, deform, elem_slot):
    cells_x, cells_y, depth = potential.shape
    elements, columns, coarse_depth = elem_slot.shape
    components, held = deform.shape
    rows = round_up(components + columns + 2, 8)
    weights = weights_of(cells_x, cells_y, columns, coarse_depth, depth, rows, components)
    across, down = lax.axis_size("gx"), lax.axis_size("gy")
    assert elements == 1 and columns % 2 == 0 and held == depth
    assert down & (down - 1) == 0 and down > 1 and 2 * cells_x == 8

    def packet(count):
        return OUT((count, depth))

    arrays = (potential, fiber_angles, deform, elem_slot)
    swaps = [[(x, x ^ 1) for x in range(across) if x ^ 1 < across]]
    upward = [(x, x + 1) for x in range(1, across - 1, 2)]
    swaps.append(upward + [(high, low) for low, high in upward])
    even, odd = pl.pallas_call(
        functools.partial(pack_x, rows=rows),
        out_shape=[packet(rows)] * 2,
        name="pack_x",
    )(potential, deform, elem_slot)
    odd = lax.ppermute(odd, "gx", swaps[1])
    even = lax.ppermute(even, "gx", swaps[0])
    rims = [flips for flips in range(1, down) if is_rim(flips)]
    side_rows = round_up(cells_x + 2, 8) + 2 * cells_x
    plain_rows = round_up(3 * components + 3, 8)
    row, plain, even_bulk, odd_bulk, *sent = pl.pallas_call(
        functools.partial(pack_y, rims=rims, rows=rows),
        out_shape=[packet(3 * rows), packet(plain_rows)]
        + [packet(3 * cells_y)] * 2
        + [packet(side_rows + plain_rows)] * len(rims),
        name="pack_y",
    )(*[IN(value) for value in arrays], IN(even), IN(odd))
    sent = dict(zip(rims, sent))
    packets = [IN(row)]
    for flips in range(1, down):
        pairs = [(y, y ^ flips) for y in range(down)]
        packets.append(IN(lax.ppermute(sent.get(flips, plain), "gy", pairs)))
    odd_bulk = lax.ppermute(odd_bulk, "gx", swaps[1])
    even_bulk = lax.ppermute(even_bulk, "gx", swaps[0])
    block = jax.ShapeDtypeStruct((cells_x, cells_y, depth), jnp.float32)
    line_count = (cells_x + 2) * cells_y + 2 * cells_x
    return pl.pallas_call(
        functools.partial(
            step,
            components=components,
            held=held,
            columns=columns,
            coarse_depth=coarse_depth,
            rows=rows,
            devices=down,
        ),
        out_shape=(block, block),
        scratch_shapes=[
            pltpu.VMEM((3 * cells_y, depth), jnp.float32),
            pltpu.VMEM((3 * cells_y, depth), jnp.float32),
            pltpu.VMEM(((columns + 2) * (elements + 2) * rows, depth), jnp.float32),
            pltpu.VMEM((components * line_count, depth), jnp.float32),
            pltpu.VMEM((6, line_count, depth), jnp.float32),
            pltpu.VMEM((cells_x * cells_y, depth), jnp.float32),
        ],
        name="step",
    )(
        IN(potential),
        IN(recovery),
        IN(fiber_angles),
        IN(even_bulk),
        IN(odd_bulk),
        weights[0],
        *[IN(value) for value in weights[1:]],
        *packets,
    )


def solution(mesh):
    placed = (
        P("gx", "gy", None),
        P("gx", "gy", None),
        P(None, "gx", "gy", None),
        P(None, ("gx", "gy")),
        P("gx", "gy", None),
    )
    return jax.shard_map(
        local,
        mesh=mesh,
        in_specs=placed,
        out_specs=(P("gx", "gy", None), P("gx", "gy", None)),
        check_vma=False,
    )
```
